32 devices in a mesh: dp: 2 (over x), ep2: 4 (over z), ep: 4 (over y, core).
Axes of the slice: x: 2, y: 2, z: 4, core: 2. Of those that a mesh axis runs over, the one named last changes fastest.
Arguments:
- tokens: bfloat16 [4096, 2560], P(('dp', 'ep2', 'ep')), parts along dimension 0
- expert_idx: int32 [4096, 6], P(('dp', 'ep2', 'ep')), parts along dimension 0
- gates: float32 [4096, 6], P(('dp', 'ep2', 'ep')), parts along dimension 0
- w_gate: bfloat16 [64, 2560, 1536], P(('ep2', 'ep'))
- w_up: bfloat16 [64, 2560, 1536], P(('ep2', 'ep'))
- w_down: bfloat16 [64, 1536, 2560], P(('ep2', 'ep'))
Outputs:
- output: bfloat16 [4096, 2560], P(('dp', 'ep2', 'ep')), parts along dimension 0
There are 2 independent parts. The reference program is written for one: setup_inputs(seed, part) draws one part's arguments, and reference() takes and returns one part's arrays. A program takes and returns all parts, laid end to end along the dimension named above; an argument that names none is the same for every part.
All inputs are finite; a program needn't handle non-finite values.
Results may differ from the reference program's by a relative error of at most 0.001.
Values are sent between devices in bfloat16 or wider.
A program may use at most 1 GiB of HBM per device.

```python
import jax
import jax.numpy as jnp
from jax import lax

GROUP_DEVS = 16
TOKENS = 128
HIDDEN = 2560
EXPERT_FF = 1536
EXPERTS = 64
TOP_K = 6

LOCAL_EXPERTS = EXPERTS // GROUP_DEVS
EXPERT_CAP = (TOKENS * TOP_K + EXPERTS - 1) // EXPERTS
TOTAL_ROWS = GROUP_DEVS * TOKENS
EXPERT_ROWS = GROUP_DEVS * EXPERT_CAP


def draw_routing(route_key):
    key_pick, key_first, key_rest, key_bias = jax.random.split(route_key, 4)
    expert_ids = jnp.arange(EXPERTS, dtype=jnp.int32)
    local_pick = jax.random.randint(key_pick, (GROUP_DEVS, GROUP_DEVS), 0, LOCAL_EXPERTS)
    picked = (expert_ids % LOCAL_EXPERTS)[None, :] == jnp.repeat(local_pick, LOCAL_EXPERTS, axis=1)
    first_score = jax.random.randint(key_first, (GROUP_DEVS, EXPERTS), 0, 1024) + 2048
    rest_score = jax.random.randint(key_rest, (GROUP_DEVS, EXPERTS), 0, 1024) + jax.random.randint(key_bias, (1, EXPERTS), 0, 512)
    score = jnp.where(picked, first_score, rest_score) * EXPERTS + expert_ids[None, :]
    sequence = jnp.argsort(-score, axis=1).astype(jnp.int32)
    positions = (jnp.arange(TOKENS)[:, None] * TOP_K + jnp.arange(TOP_K)[None, :]) % EXPERTS
    chosen = jnp.take(sequence, positions.reshape(-1), axis=1)
    return chosen.reshape(TOTAL_ROWS, TOP_K)


def setup_inputs(seed: int = 0, part: int = 0) -> dict:
    root_key = jax.random.key(seed)
    shared_key, local_root = jax.random.split(root_key)
    part_key = jax.random.fold_in(local_root, part)
    key_tok, key_route, key_gate = jax.random.split(part_key, 3)
    key_wg, key_wu, key_wd = jax.random.split(shared_key, 3)
    tokens = jax.random.normal(key_tok, (TOTAL_ROWS, HIDDEN), jnp.float32).astype(jnp.bfloat16)
    expert_idx = draw_routing(key_route)
    gate_logits = jax.random.normal(key_gate, (TOTAL_ROWS, TOP_K), jnp.float32)
    gates = 0.5 * TOP_K * jax.nn.softmax(gate_logits, axis=-1)
    w_gate = (jax.random.normal(key_wg, (EXPERTS, HIDDEN, EXPERT_FF), jnp.float32) * HIDDEN ** -0.5).astype(jnp.bfloat16)
    w_up = (jax.random.normal(key_wu, (EXPERTS, HIDDEN, EXPERT_FF), jnp.float32) * HIDDEN ** -0.5).astype(jnp.bfloat16)
    w_down = (jax.random.normal(key_wd, (EXPERTS, EXPERT_FF, HIDDEN), jnp.float32) * EXPERT_FF ** -0.5).astype(jnp.bfloat16)
    return {'tokens': tokens, 'expert_idx': expert_idx, 'gates': gates, 'w_gate': w_gate, 'w_up': w_up, 'w_down': w_down}


def expert_ffn(operands):
    rows_in, gate_w, up_w, down_w = operands
    act_gate = jnp.dot(rows_in, gate_w, preferred_element_type=jnp.float32)
    act_up = jnp.dot(rows_in, up_w, preferred_element_type=jnp.float32)
    inner_act = (jax.nn.silu(act_gate) * act_up).astype(jnp.bfloat16)
    return jnp.dot(inner_act, down_w, preferred_element_type=jnp.float32).astype(jnp.bfloat16)


def reference(tokens, expert_idx, gates, w_gate, w_up, w_down):
    flat_ids = expert_idx.reshape(-1)
    n_items = flat_ids.shape[0]
    sort_order = jnp.argsort(flat_ids, stable=True)
    sorted_ids = flat_ids[sort_order]
    counts = jnp.bincount(flat_ids, length=EXPERTS)
    starts = jnp.cumsum(counts) - counts
    rank_sorted = (jnp.arange(n_items) - starts[sorted_ids]).astype(jnp.int32)
    slot_rank = jnp.zeros((n_items,), jnp.int32).at[sort_order].set(rank_sorted)
    token_of = jnp.arange(n_items) // TOP_K
    expert_in = jnp.zeros((EXPERTS, EXPERT_ROWS, HIDDEN), tokens.dtype).at[flat_ids, slot_rank].set(tokens[token_of])
    expert_out = lax.map(expert_ffn, (expert_in, w_gate, w_up, w_down))
    routed = expert_out[flat_ids, slot_rank].reshape(TOTAL_ROWS, TOP_K, HIDDEN)
    mixed = jnp.sum(gates[:, :, None] * routed.astype(jnp.float32), axis=1)
    return (tokens.astype(jnp.float32) + mixed).astype(jnp.bfloat16)
```

```python
import functools

import jax
import jax.numpy as jnp
from jax import lax
from jax.experimental import pallas as pl
from jax.experimental.pallas import tpu as pltpu
from jax.sharding import PartitionSpec as P

MESH = pl.DeviceIdType.MESH
BF = jnp.bfloat16
F32 = jnp.float32
NZ = 4
NE = 4
NDEV = NZ * NE
LE = 4
CAP = 12
BLK = LE * CAP
PLANE = NE * BLK
HALF = BLK // 2
WINDOWS = (0, 8, 24, 32)
FC = 512
DC = 512
NG = 5
ND = 6


def iota(shape, dim):
    return lax.broadcasted_iota(jnp.int32, shape, dim)


def div_cap(v):
    return (v * 43691) >> 19


def piece(e, desc):
    base = (e // 2) * HALF
    if desc:
        return (base + 16, 8) if e % 2 else (base, 16)
    return (base + 8, 16) if e % 2 else (base, 8)


def kernel(tok, idx, gates, wg, wu, wd, out, xl, idxl, sel, xr, a_buf, h_buf, ys, yr, gm, acc, gu, wdb,
           gsem, dsem, isend, irecv, lsend, lrecv, ssend, srecv, ysend, yrecv):
    T, D = tok.shape
    F = wg.shape[2]
    n_f, n_d = F // FC, D // DC
    dp, z, ep = lax.axis_index("dp"), lax.axis_index("ep2"), lax.axis_index("ep")
    me = z * NE + ep
    low = z < NZ // 2
    inner = (z == 1) | (z == 2)
    near = jnp.where(low, 1 - z, 5 - z)
    far1 = jnp.where(low, 2, 1)
    far2 = jnp.where(low, 3, 0)

    def remote(src, dst, ss, rs, zz, ee):
        return pltpu.make_async_remote_copy(
            src_ref=src, dst_ref=dst, send_sem=ss, recv_sem=rs, device_id=(dp, zz, ee), device_id_type=MESH
        )

    def gu_copies(i):
        e, c, slot = lax.div(i, n_f), lax.rem(i, n_f), lax.rem(i, NG)
        cols = pl.ds(pl.multiple_of(c * FC, FC), FC)
        return (
            pltpu.make_async_copy(wg.at[e, :, cols], gu.at[slot, 0], gsem.at[slot, 0]),
            pltpu.make_async_copy(wu.at[e, :, cols], gu.at[slot, 1], gsem.at[slot, 1]),
        )

    def d_copies(i):
        e, c, slot = lax.div(i, n_d), lax.rem(i, n_d), lax.rem(i, ND)
        cols = pl.ds(pl.multiple_of(c * DC, DC), DC)
        return (pltpu.make_async_copy(wd.at[e, :, cols], wdb.at[slot], dsem.at[slot]),)

    for i in range(NG):
        for cp in gu_copies(jnp.int32(i)):
            cp.start()
    for i in range(ND):
        for cp in d_copies(jnp.int32(i)):
            cp.start()

    barrier = pltpu.get_barrier_semaphore()
    for k in range(1, NDEV):
        peer = lax.rem(me + k, NDEV)
        pl.semaphore_signal(barrier, inc=1, device_id=(dp, lax.div(peer, NE), lax.rem(peer, NE)), device_id_type=MESH)
    pl.semaphore_wait(barrier, NDEV - 1)

    def line(b, n, to):
        return remote(xl.at[b], xl.at[b], lsend.at[n], lrecv.at[b], to, ep)

    def line_own(n, to):
        return remote(tok, xl.at[z], lsend.at[n], lrecv.at[z], to, ep)

    def line_wait(b):
        line(b, 0, z).wait_recv()

    def icopy(k):
        return remote(idx, idxl.at[z], isend.at[k - 1], irecv.at[z], lax.rem(z + k, NZ), ep)

    @pl.when(inner)
    def _():
        line_own(0, far1).start()

    line_own(1, near).start()
    for k in range(1, NZ):
        icopy(k).start()
    idxl[z] = idx[...]
    xl[z] = tok[...]

    upper = jnp.where(iota((T, T), 0) < iota((T, T), 1), 1.0, 0.0).astype(BF)

    def codes(ids, first, n):
        eid = iota((n, T), 0) + first
        hit = jnp.zeros((n, T), F32)
        for j in range(6):
            hit = hit + jnp.where(ids[j : j + 1, :] == eid, 1.0, 0.0)
        rank = jnp.dot(hit.astype(BF), upper, preferred_element_type=F32)
        return jnp.where(hit > 0.5, rank, -1.0).astype(BF)

    def s_copy(b, k):
        d = lax.rem(ep + k, NE)
        return remote(sel.at[b, d], xr.at[b * NE + ep], ssend.at[b, k - 1], srecv.at[b * NE + ep], z, d)

    def select(b):
        code = codes(idxl[b], z * NE * LE, NE * LE)
        r = iota((PLANE, NE * LE), 0)
        ex = jnp.where(div_cap(r) == iota((PLANE, NE * LE), 1), 1.0, 0.0).astype(BF)
        code_r = jnp.dot(ex, code, preferred_element_type=F32)
        r = iota((PLANE, T), 0)
        slot = (r - div_cap(r) * CAP).astype(F32)
        pick = jnp.where(code_r == slot, 1.0, 0.0).astype(BF)

        def cols(c, _):
            cs = pl.ds(pl.multiple_of(c * DC, DC), DC)
            rows = jnp.dot(pick, xl[b, :, cs], preferred_element_type=F32).astype(BF)
            sel[b, :, :, cs] = rows.reshape(NE, BLK, DC)
            return 0

        lax.fori_loop(0, n_d, cols, 0)
        for k in range(1, NE):
            s_copy(b, k).start()
        xr[b * NE + ep] = sel[b, ep]

    def idx_wait(b):
        remote(idx, idxl.at[b], isend.at[0], irecv.at[b], z, ep).wait_recv()

    select(z)

    n_exp = NDEV * LE
    idx_v, gates_v = idx[...], gates[...]
    code = codes(idx_v, 0, n_exp)
    eid = iota((n_exp, T), 0)
    gate = jnp.zeros((n_exp, T), F32)
    for j in range(6):
        gate = gate + jnp.where(idx_v[j : j + 1, :] == eid, gates_v[j : j + 1, :], 0.0)
    g_hi = gate.astype(BF)
    rest = gate - g_hi.astype(F32)
    g_mid = rest.astype(BF)
    g_lo = (rest - g_mid.astype(F32)).astype(BF)

    def spread(a, ex):
        return lax.dot_general(a, ex, (((0,), (0,)), ((), ())), preferred_element_type=F32)

    for b in range(NZ):
        c = iota((n_exp, PLANE), 1)
        ex = jnp.where(div_cap(c) + b * NE * LE == iota((n_exp, PLANE), 0), 1.0, 0.0).astype(BF)
        c = iota((T, PLANE), 1)
        slot = (c - div_cap(c) * CAP).astype(F32)
        on = spread(code, ex) == slot
        for q, part in enumerate((g_hi, g_mid, g_lo)):
            gm[q, b] = jnp.where(on, spread(part, ex), 0.0).astype(BF)

    def pick_plane(a, b):
        return jnp.where(inner, a, b)

    q0, q1, q2 = pick_plane(far1, near), pick_plane(far2, far1), pick_plane(near, far2)
    line_wait(q0)

    @pl.when(inner)
    def _():
        line(far1, 2, near).start()
        line_wait(near)
        line(near, 3, far1).start()

    idx_wait(q0)
    select(q0)
    line_wait(q1)

    @pl.when(inner)
    def _():
        line(far2, 4, near).start()

    idx_wait(q1)
    select(q1)

    def rows_wait(b):
        for k in range(1, NE):
            i = b * NE + lax.rem(ep + k, NE)
            remote(xr.at[i], xr.at[i], ssend.at[0, 0], srecv.at[i], z, ep).wait_recv()

    def y_copy(zz, ee, e, desc):
        m = zz * NE + ee
        rows = pl.ds(*piece(e, desc))
        return remote(ys.at[m, rows], yr.at[me, rows], ysend.at[e, m], yrecv.at[e, me], zz, ee)

    def experts(p0, p1, n_pass):
        desc = n_pass == 1
        rows_wait(p0)

        @pl.when(p1 != p0)
        def _():
            rows_wait(p1)

        def step(i, ring, total, copies, before):
            if before:
                if n_pass == 0:
                    for cp in copies(i):
                        cp.wait()
                else:
                    @pl.when(i < total - ring if desc else i >= ring)
                    def _():
                        for cp in copies(i):
                            cp.wait()
            else:
                nxt = i - ring if desc else i + ring

                @pl.when(nxt >= 0 if desc else nxt < total)
                def _():
                    for cp in copies(nxt):
                        cp.start()

        for e in reversed(range(LE)) if desc else range(LE):
            win = WINDOWS[e]
            for s, p in enumerate((p0, p1)):
                def gather(m, _, s=s, p=p):
                    rows = pl.ds(pl.multiple_of(s * NE * 16 + m * 16, 16), 16)
                    a_buf[rows, :] = xr[p * NE + m, win : win + 16, :]
                    return 0

                lax.fori_loop(0, NE, gather, 0)

            def gate_up(c, _):
                c = n_f - 1 - c if desc else c
                i = e * n_f + c
                slot = lax.rem(i, NG)
                step(i, NG, LE * n_f, gu_copies, True)
                a = a_buf[...]
                g = jnp.dot(a, gu[slot, 0], preferred_element_type=F32)
                u = jnp.dot(a, gu[slot, 1], preferred_element_type=F32)
                h_buf[:, pl.ds(pl.multiple_of(c * FC, FC), FC)] = (jax.nn.silu(g) * u).astype(BF)
                step(i, NG, LE * n_f, gu_copies, False)
                return 0

            lax.fori_loop(0, n_f, gate_up, 0)

            def down_proj(c, _):
                c = n_d - 1 - c if desc else c
                i = e * n_d + c
                slot = lax.rem(i, ND)
                step(i, ND, LE * n_d, d_copies, True)
                y = jnp.dot(h_buf[...], wdb[slot], preferred_element_type=F32).reshape(2, NE, 16, DC)
                cs = pl.ds(pl.multiple_of(c * DC, DC), DC)
                second = (e % 2 == 0) == desc
                for s, p in enumerate((p0, p1)):
                    to = pl.ds(p * NE, NE)
                    if not second:
                        ys[to, win : win + 16, cs] = y[s].astype(BF)
                    elif e % 2:
                        old = ys[to, win : win + 8, cs].astype(F32)
                        keep = iota((NE, 8, DC), 1) < 4
                        ys[to, win : win + 8, cs] = jnp.where(keep, old, y[s, :, :8]).astype(BF)
                        ys[to, win + 8 : win + 16, cs] = y[s, :, 8:].astype(BF)
                    else:
                        old = ys[to, win + 8 : win + 16, cs].astype(F32)
                        keep = iota((NE, 8, DC), 1) >= 4
                        ys[to, win + 8 : win + 16, cs] = jnp.where(keep, old, y[s, :, 8:]).astype(BF)
                        ys[to, win : win + 8, cs] = y[s, :, :8].astype(BF)
                step(i, ND, LE * n_d, d_copies, False)
                return 0

            lax.fori_loop(0, n_d, down_proj, 0)

            @pl.when(p1 != p0)
            def _():
                for k in range(NE):
                    y_copy(p1, k, e, desc).start()

            for k in range(NE):
                @pl.when((p0 != z) | (k != ep))
                def _(k=k):
                    y_copy(p0, k, e, desc).start()

    experts(pick_plane(far1, z), pick_plane(far1, near), 0)

    @pl.when(jnp.logical_not(inner))
    def _():
        line_wait(q2)

    idx_wait(q2)
    select(q2)
    experts(pick_plane(far2, far1), pick_plane(far2, far1), 1)
    experts(pick_plane(z, far2), pick_plane(near, far2), 2)

    yr[me] = ys[me]

    def y_wait(i, desc):
        for e in range(LE):
            rows = pl.ds(*piece(e, desc))
            remote(yr.at[i, rows], yr.at[i, rows], ysend.at[0, 0], yrecv.at[e, i], z, ep).wait_recv()

    for n, b in enumerate((z, near, far1, far2)):
        second = jnp.abs(b - z) == 2
        for k in range(1 if n == 0 else 0, NE):
            i = b * NE + (lax.rem(ep + k, NE) if n == 0 else k)
            if n < 2:
                y_wait(i, False)
            else:
                @pl.when(second)
                def _(i=i):
                    y_wait(i, True)

                @pl.when(jnp.logical_not(second))
                def _(i=i):
                    y_wait(i, False)

        def mix(c, _):
            cs = pl.ds(pl.multiple_of(c * DC, DC), DC)
            rows = yr[pl.ds(b * NE, NE), :, cs].reshape(PLANE, DC)
            s = tok[:, cs].astype(F32) if n == 0 else acc[:, cs]
            for q in range(3):
                s = s + jnp.dot(gm[q, b], rows, preferred_element_type=F32)
            if n < NZ - 1:
                acc[:, cs] = s
            else:
                out[:, cs] = s.astype(BF)
            return 0

        lax.fori_loop(0, n_d, mix, 0)

    for k in range(1, NZ):
        icopy(k).wait_send()
    for b in range(NZ):
        for k in range(1, NE):
            s_copy(b, k).wait_send()
    line_own(1, near).wait_send()

    @pl.when(inner)
    def _():
        line_own(0, far1).wait_send()
        line(far1, 2, near).wait_send()
        line(near, 3, far1).wait_send()
        line(far2, 4, near).wait_send()

    for b in (z, near, far1, far2):
        second = jnp.abs(b - z) == 2
        for k in range(NE):
            for desc in (False, True):
                @pl.when((second if desc else jnp.logical_not(second)) & ((b != z) | (k != ep)))
                def _(b=b, k=k, desc=desc):
                    for e in range(LE):
                        y_copy(b, k, e, desc).wait_send()


def solution(mesh):
    row_spec = P(('dp', 'ep2', 'ep'), None)
    weight_spec = P(('ep2', 'ep'), None, None)

    def local_step(tokens, expert_idx, gates, w_gate, w_up, w_down):
        T, D = tokens.shape
        F = w_gate.shape[2]
        vm = pl.BlockSpec(memory_space=pltpu.VMEM)
        hbm = pl.BlockSpec(memory_space=pl.ANY)
        dma = pltpu.SemaphoreType.DMA
        return pl.pallas_call(
            kernel,
            name="moe",
            out_shape=jax.ShapeDtypeStruct((T, D), BF),
            in_specs=[vm, vm, vm, hbm, hbm, hbm],
            out_specs=vm,
            scratch_shapes=[
                pltpu.VMEM((NZ, T, D), BF),
                pltpu.VMEM((NZ, 6, T), jnp.int32),
                pltpu.VMEM((NZ, NE, BLK, D), BF),
                pltpu.VMEM((NDEV, BLK, D), BF),
                pltpu.VMEM((2 * NE * 16, D), BF),
                pltpu.VMEM((2 * NE * 16, F), BF),
                pltpu.VMEM((NDEV, BLK, D), BF),
                pltpu.VMEM((NDEV, BLK, D), BF),
                pltpu.VMEM((3, NZ, T, PLANE), BF),
                pltpu.VMEM((T, D), F32),
                pltpu.VMEM((NG, 2, D, FC), BF),
                pltpu.VMEM((ND, F, DC), BF),
                dma((NG, 2)),
                dma((ND,)),
                dma((NZ - 1,)),
                dma((NZ,)),
                dma((5,)),
                dma((NZ,)),
                dma((NZ, NE - 1)),
                dma((NDEV,)),
                dma((LE, NDEV)),
                dma((LE, NDEV)),
            ],
            compiler_params=pltpu.CompilerParams(
                collective_id=0, has_side_effects=True, vmem_limit_bytes=67043328
            ),
        )(tokens, expert_idx.T, gates.T, w_gate, w_up, w_down)

    return jax.shard_map(local_step, mesh=mesh, in_specs=(row_spec, row_spec, row_spec, weight_spec, weight_spec, weight_spec), out_specs=row_spec, check_vma=False)
```

```python
import functools

import jax
import jax.numpy as jnp
from jax import lax
from jax.experimental import pallas as pl
from jax.experimental.pallas import tpu as pltpu
from jax.sharding import PartitionSpec as P

MESH = pl.DeviceIdType.MESH
BF = jnp.bfloat16
F32 = jnp.float32
NZ = 4
NE = 4
NDEV = NZ * NE
LE = 4
CAP = 12
BLK = LE * CAP
PLANE = NE * BLK
HALF = BLK // 2
WINDOWS = (0, 8, 24, 32)
FC = 512
DC = 512
NG = 5
ND = 6


def iota(shape, dim):
    return lax.broadcasted_iota(jnp.int32, shape, dim)


def div_cap(v):
    return (v * 43691) >> 19


def piece(e, desc):
    base = (e // 2) * HALF
    if desc:
        return (base + 16, 8) if e % 2 else (base, 16)
    return (base + 8, 16) if e % 2 else (base, 8)


def kernel(tok, idx, gates, wg, wu, wd, out, xl, idxl, sel, xr, a_buf, h_buf, ys, yr, gm, acc, gu, wdb,
           gsem, dsem, isend, irecv, lsend, lrecv, ssend, srecv, ysend, yrecv):
    T, D = tok.shape
    F = wg.shape[2]
    n_f, n_d = F // FC, D // DC
    dp, z, ep = lax.axis_index("dp"), lax.axis_index("ep2"), lax.axis_index("ep")
    me = z * NE + ep
    low = z < NZ // 2
    inner = (z == 1) | (z == 2)
    near = jnp.where(low, 1 - z, 5 - z)
    far1 = jnp.where(low, 2, 1)
    far2 = jnp.where(low, 3, 0)

    def remote(src, dst, ss, rs, zz, ee):
        return pltpu.make_async_remote_copy(
            src_ref=src, dst_ref=dst, send_sem=ss, recv_sem=rs, device_id=(dp, zz, ee), device_id_type=MESH
        )

    def gu_copies(i):
        e, c, slot = lax.div(i, n_f), lax.rem(i, n_f), lax.rem(i, NG)
        cols = pl.ds(pl.multiple_of(c * FC, FC), FC)
        return (
            pltpu.make_async_copy(wg.at[e, :, cols], gu.at[slot, 0], gsem.at[slot, 0]),
            pltpu.make_async_copy(wu.at[e, :, cols], gu.at[slot, 1], gsem.at[slot, 1]),
        )

    def d_copies(i):
        e, c, slot = lax.div(i, n_d), lax.rem(i, n_d), lax.rem(i, ND)
        cols = pl.ds(pl.multiple_of(c * DC, DC), DC)
        return (pltpu.make_async_copy(wd.at[e, :, cols], wdb.at[slot], dsem.at[slot]),)

    for i in range(NG):
        for cp in gu_copies(jnp.int32(i)):
            cp.start()
    for i in range(ND):
        for cp in d_copies(jnp.int32(i)):
            cp.start()

    barrier = pltpu.get_barrier_semaphore()
    for k in range(1, NDEV):
        peer = lax.rem(me + k, NDEV)
        pl.semaphore_signal(barrier, inc=1, device_id=(dp, lax.div(peer, NE), lax.rem(peer, NE)), device_id_type=MESH)
    pl.semaphore_wait(barrier, NDEV - 1)

    def line(b, n, to):
        return remote(xl.at[b], xl.at[b], lsend.at[n], lrecv.at[b], to, ep)

    def line_own(n, to):
        return remote(tok, xl.at[z], lsend.at[n], lrecv.at[z], to, ep)

    def line_wait(b):
        line(b, 0, z).wait_recv()

    def icopy(k):
        return remote(idx, idxl.at[z], isend.at[k - 1], irecv.at[z], lax.rem(z + k, NZ), ep)

    @pl.when(inner)
    def _():
        line_own(0, far1).start()

    line_own(1, near).start()
    for k in range(1, NZ):
        icopy(k).start()
    idxl[z] = idx[...]
    xl[z] = tok[...]

    upper = jnp.where(iota((T, T), 0) < iota((T, T), 1), 1.0, 0.0).astype(BF)

    def codes(ids, first, n):
        eid = iota((n, T), 0) + first
        hit = jnp.zeros((n, T), F32)
        for j in range(6):
            hit = hit + jnp.where(ids[j : j + 1, :] == eid, 1.0, 0.0)
        rank = jnp.dot(hit.astype(BF), upper, preferred_element_type=F32)
        return jnp.where(hit > 0.5, rank, -1.0).astype(BF)

    def s_copy(b, k):
        d = lax.rem(ep + k, NE)
        return remote(sel.at[b, d], xr.at[b * NE + ep], ssend.at[b, k - 1], srecv.at[b * NE + ep], z, d)

    def select(b):
        code = codes(idxl[b], z * NE * LE, NE * LE)
        r = iota((PLANE, NE * LE), 0)
        ex = jnp.where(div_cap(r) == iota((PLANE, NE * LE), 1), 1.0, 0.0).astype(BF)
        code_r = jnp.dot(ex, code, preferred_element_type=F32)
        r = iota((PLANE, T), 0)
        slot = (r - div_cap(r) * CAP).astype(F32)
        pick = jnp.where(code_r == slot, 1.0, 0.0).astype(BF)

        def cols(c, _):
            cs = pl.ds(pl.multiple_of(c * DC, DC), DC)
            rows = jnp.dot(pick, xl[b, :, cs], preferred_element_type=F32).astype(BF)
            sel[b, :, :, cs] = rows.reshape(NE, BLK, DC)
            return 0

        lax.fori_loop(0, n_d, cols, 0)
        for k in range(1, NE):
            s_copy(b, k).start()
        xr[b * NE + ep] = sel[b, ep]

    def idx_wait(b):
        remote(idx, idxl.at[b], isend.at[0], irecv.at[b], z, ep).wait_recv()

    select(z)

    n_exp = NDEV * LE
    idx_v, gates_v = idx[...], gates[...]
    code = codes(idx_v, 0, n_exp)
    eid = iota((n_exp, T), 0)
    gate = jnp.zeros((n_exp, T), F32)
    for j in range(6):
        gate = gate + jnp.where(idx_v[j : j + 1, :] == eid, gates_v[j : j + 1, :], 0.0)
    g_hi = gate.astype(BF)
    rest = gate - g_hi.astype(F32)
    g_mid = rest.astype(BF)
    g_lo = (rest - g_mid.astype(F32)).astype(BF)

    def spread(a, ex):
        return lax.dot_general(a, ex, (((0,), (0,)), ((), ())), preferred_element_type=F32)

    for b in range(NZ):
        c = iota((n_exp, PLANE), 1)
        ex = jnp.where(div_cap(c) + b * NE * LE == iota((n_exp, PLANE), 0), 1.0, 0.0).astype(BF)
        c = iota((T, PLANE), 1)
        slot = (c - div_cap(c) * CAP).astype(F32)
        on = spread(code, ex) == slot
        for q, part in enumerate((g_hi, g_mid, g_lo)):
            gm[q, b] = jnp.where(on, spread(part, ex), 0.0).astype(BF)

    def pick_plane(a, b):
        return jnp.where(inner, a, b)

    q0, q1, q2 = pick_plane(far1, near), pick_plane(far2, far1), pick_plane(near, far2)
    line_wait(q0)

    @pl.when(inner)
    def _():
        line(far1, 2, near).start()
        line_wait(near)
        line(near, 3, far1).start()

    idx_wait(q0)
    select(q0)
    line_wait(q1)

    @pl.when(inner)
    def _():
        line(far2, 4, near).start()

    idx_wait(q1)
    select(q1)

    def last_block():
        @pl.when(jnp.logical_not(inner))
        def _():
            line_wait(q2)

        idx_wait(q2)
        select(q2)

    pl.when(inner)(last_block)

    def rows_wait(b):
        for k in range(1, NE):
            i = b * NE + lax.rem(ep + k, NE)
            remote(xr.at[i], xr.at[i], ssend.at[0, 0], srecv.at[i], z, ep).wait_recv()

    def y_copy(zz, ee, e, desc):
        m = zz * NE + ee
        rows = pl.ds(*piece(e, desc))
        return remote(ys.at[m, rows], yr.at[me, rows], ysend.at[e, m], yrecv.at[e, me], zz, ee)

    def experts(p0, p1, n_pass):
        desc = n_pass == 1
        rows_wait(p0)
        rows_wait(p1)

        def step(i, ring, total, copies, before):
            if before:
                if n_pass == 0:
                    for cp in copies(i):
                        cp.wait()
                else:
                    @pl.when(i < total - ring if desc else i >= ring)
                    def _():
                        for cp in copies(i):
                            cp.wait()
            else:
                nxt = i - ring if desc else i + ring

                @pl.when(nxt >= 0 if desc else nxt < total)
                def _():
                    for cp in copies(nxt):
                        cp.start()

        for e in reversed(range(LE)) if desc else range(LE):
            win = WINDOWS[e]
            for s, p in enumerate((p0, p1)):
                def gather(m, _, s=s, p=p):
                    rows = pl.ds(pl.multiple_of(s * NE * 16 + m * 16, 16), 16)
                    a_buf[rows, :] = xr[p * NE + m, win : win + 16, :]
                    return 0

                lax.fori_loop(0, NE, gather, 0)

            def gate_up(c, _):
                c = n_f - 1 - c if desc else c
                i = e * n_f + c
                slot = lax.rem(i, NG)
                step(i, NG, LE * n_f, gu_copies, True)
                a = a_buf[...]
                g = jnp.dot(a, gu[slot, 0], preferred_element_type=F32)
                u = jnp.dot(a, gu[slot, 1], preferred_element_type=F32)
                h_buf[:, pl.ds(pl.multiple_of(c * FC, FC), FC)] = (jax.nn.silu(g) * u).astype(BF)
                step(i, NG, LE * n_f, gu_copies, False)
                return 0

            lax.fori_loop(0, n_f, gate_up, 0)

            def down_proj(c, _):
                c = n_d - 1 - c if desc else c
                i = e * n_d + c
                slot = lax.rem(i, ND)
                step(i, ND, LE * n_d, d_copies, True)
                y = jnp.dot(h_buf[...], wdb[slot], preferred_element_type=F32).reshape(2, NE, 16, DC)
                cs = pl.ds(pl.multiple_of(c * DC, DC), DC)
                second = (e % 2 == 0) == desc
                for s, p in enumerate((p0, p1)):
                    to = pl.ds(p * NE, NE)
                    if not second:
                        ys[to, win : win + 16, cs] = y[s].astype(BF)
                    elif e % 2:
                        old = ys[to, win : win + 8, cs].astype(F32)
                        keep = iota((NE, 8, DC), 1) < 4
                        ys[to, win : win + 8, cs] = jnp.where(keep, old, y[s, :, :8]).astype(BF)
                        ys[to, win + 8 : win + 16, cs] = y[s, :, 8:].astype(BF)
                    else:
                        old = ys[to, win + 8 : win + 16, cs].astype(F32)
                        keep = iota((NE, 8, DC), 1) >= 4
                        ys[to, win + 8 : win + 16, cs] = jnp.where(keep, old, y[s, :, 8:]).astype(BF)
                        ys[to, win : win + 8, cs] = y[s, :, :8].astype(BF)
                step(i, ND, LE * n_d, d_copies, False)
                return 0

            lax.fori_loop(0, n_d, down_proj, 0)

            for k in range(NE):
                y_copy(p0, k, e, desc).start()
            if n_pass:
                for k in range(NE):
                    y_copy(p1, k, e, desc).start()
            elif e == LE - 2:
                pl.when(jnp.logical_not(inner))(last_block)
        if n_pass == 0:
            for e in range(LE):
                for k in range(1, NE):
                    y_copy(z, lax.rem(ep + k, NE), e, desc).start()

    experts(pick_plane(far1, near), z, 0)
    experts(far2, pick_plane(near, far1), 1)

    yr[me] = ys[me]

    def y_wait(i, desc):
        for e in range(LE):
            rows = pl.ds(*piece(e, desc))
            remote(yr.at[i, rows], yr.at[i, rows], ysend.at[0, 0], yrecv.at[e, i], z, ep).wait_recv()

    edge = jnp.logical_not(inner)
    for n, b in enumerate((z, near, far1, far2)):
        for k in range(1 if n == 0 else 0, NE):
            i = b * NE + (lax.rem(ep + k, NE) if n == 0 else k)
            if n in (0, 3):
                y_wait(i, n == 3)
            else:
                @pl.when(edge)
                def _(i=i):
                    y_wait(i, True)

                @pl.when(inner)
                def _(i=i):
                    y_wait(i, False)

        def mix(c, _):
            cs = pl.ds(pl.multiple_of(c * DC, DC), DC)
            rows = yr[pl.ds(b * NE, NE), :, cs].reshape(PLANE, DC)
            s = tok[:, cs].astype(F32) if n == 0 else acc[:, cs]
            for q in range(3):
                s = s + jnp.dot(gm[q, b], rows, preferred_element_type=F32)
            if n < NZ - 1:
                acc[:, cs] = s
            else:
                out[:, cs] = s.astype(BF)
            return 0

        lax.fori_loop(0, n_d, mix, 0)

    for k in range(1, NZ):
        icopy(k).wait_send()
    for b in range(NZ):
        for k in range(1, NE):
            s_copy(b, k).wait_send()
    line_own(1, near).wait_send()

    @pl.when(inner)
    def _():
        line_own(0, far1).wait_send()
        line(far1, 2, near).wait_send()
        line(near, 3, far1).wait_send()
        line(far2, 4, near).wait_send()

    def sent(b, k, desc):
        for e in range(LE):
            y_copy(b, k, e, desc).wait_send()

    for k in range(NE):
        if k:
            sent(z, lax.rem(ep + k, NE), False)
        sent(far2, k, True)
        for desc in (False, True):
            @pl.when(inner)
            def _(k=k, desc=desc):
                sent(near if desc else far1, k, desc)

            @pl.when(edge)
            def _(k=k, desc=desc):
                sent(far1 if desc else near, k, desc)


def solution(mesh):
    row_spec = P(('dp', 'ep2', 'ep'), None)
    weight_spec = P(('ep2', 'ep'), None, None)

    def local_step(tokens, expert_idx, gates, w_gate, w_up, w_down):
        T, D = tokens.shape
        F = w_gate.shape[2]
        vm = pl.BlockSpec(memory_space=pltpu.VMEM)
        hbm = pl.BlockSpec(memory_space=pl.ANY)
        dma = pltpu.SemaphoreType.DMA
        return pl.pallas_call(
            kernel,
            name="moe",
            out_shape=jax.ShapeDtypeStruct((T, D), BF),
            in_specs=[vm, vm, vm, hbm, hbm, hbm],
            out_specs=vm,
            scratch_shapes=[
                pltpu.VMEM((NZ, T, D), BF),
                pltpu.VMEM((NZ, 6, T), jnp.int32),
                pltpu.VMEM((NZ, NE, BLK, D), BF),
                pltpu.VMEM((NDEV, BLK, D), BF),
                pltpu.VMEM((2 * NE * 16, D), BF),
                pltpu.VMEM((2 * NE * 16, F), BF),
                pltpu.VMEM((NDEV, BLK, D), BF),
                pltpu.VMEM((NDEV, BLK, D), BF),
                pltpu.VMEM((3, NZ, T, PLANE), BF),
                pltpu.VMEM((T, D), F32),
                pltpu.VMEM((NG, 2, D, FC), BF),
                pltpu.VMEM((ND, F, DC), BF),
                dma((NG, 2)),
                dma((ND,)),
                dma((NZ - 1,)),
                dma((NZ,)),
                dma((5,)),
                dma((NZ,)),
                dma((NZ, NE - 1)),
                dma((NDEV,)),
                dma((LE, NDEV)),
                dma((LE, NDEV)),
            ],
            compiler_params=pltpu.CompilerParams(
                collective_id=0, has_side_effects=True, vmem_limit_bytes=67043328
            ),
        )(tokens, expert_idx.T, gates.T, w_gate, w_up, w_down)

    return jax.shard_map(local_step, mesh=mesh, in_specs=(row_spec, row_spec, row_spec, weight_spec, weight_spec, weight_spec), out_specs=row_spec, check_vma=False)
```

```python
import functools

import jax
import jax.numpy as jnp
from jax import lax
from jax.experimental import pallas as pl
from jax.experimental.pallas import tpu as pltpu
from jax.sharding import PartitionSpec as P

MESH = pl.DeviceIdType.MESH
BF = jnp.bfloat16
F32 = jnp.float32
NZ = 4
NE = 4
NDEV = NZ * NE
LE = 4
CAP = 12
BLK = LE * CAP
PLANE = NE * BLK
HALF = BLK // 2
WINDOWS = (0, 8, 24, 32)
FC = 512
DC = 512
NG = 5
ND = 6


def iota(shape, dim):
    return lax.broadcasted_iota(jnp.int32, shape, dim)


def div_cap(v):
    return (v * 43691) >> 19


def piece(e, desc):
    base = (e // 2) * HALF
    if desc:
        return (base + 16, 8) if e % 2 else (base, 16)
    return (base + 8, 16) if e % 2 else (base, 8)


def kernel(tok, idx, gates, wg, wu, wd, out, xl, idxl, sel, xr, a_buf, h_buf, ys, yr, gm, acc, gu, wdb,
           gsem, dsem, isend, irecv, lsend, lrecv, ssend, srecv, ysend, yrecv):
    T, D = tok.shape
    F = wg.shape[2]
    n_f, n_d = F // FC, D // DC
    dp, z, ep = lax.axis_index("dp"), lax.axis_index("ep2"), lax.axis_index("ep")
    me = z * NE + ep
    low = z < NZ // 2
    inner = (z == 1) | (z == 2)
    edge = jnp.logical_not(inner)
    near = jnp.where(low, 1 - z, 5 - z)
    far1 = jnp.where(low, 2, 1)
    far2 = jnp.where(low, 3, 0)

    def remote(src, dst, ss, rs, zz, ee):
        return pltpu.make_async_remote_copy(
            src_ref=src, dst_ref=dst, send_sem=ss, recv_sem=rs, device_id=(dp, zz, ee), device_id_type=MESH
        )

    def gu_copies(i):
        e, c, slot = lax.div(i, n_f), lax.rem(i, n_f), lax.rem(i, NG)
        cols = pl.ds(pl.multiple_of(c * FC, FC), FC)
        return (
            pltpu.make_async_copy(wg.at[e, :, cols], gu.at[slot, 0], gsem.at[slot, 0]),
            pltpu.make_async_copy(wu.at[e, :, cols], gu.at[slot, 1], gsem.at[slot, 1]),
        )

    def d_copies(i):
        e, c, slot = lax.div(i, n_d), lax.rem(i, n_d), lax.rem(i, ND)
        cols = pl.ds(pl.multiple_of(c * DC, DC), DC)
        return (pltpu.make_async_copy(wd.at[e, :, cols], wdb.at[slot], dsem.at[slot]),)

    for i in range(NG):
        for cp in gu_copies(jnp.int32(i)):
            cp.start()
    for i in range(ND):
        for cp in d_copies(jnp.int32(i)):
            cp.start()

    barrier = pltpu.get_barrier_semaphore()
    for k in range(1, NDEV):
        peer = lax.rem(me + k, NDEV)
        pl.semaphore_signal(barrier, inc=1, device_id=(dp, lax.div(peer, NE), lax.rem(peer, NE)), device_id_type=MESH)
    pl.semaphore_wait(barrier, NDEV - 1)

    def line(b, n, to):
        return remote(xl.at[b], xl.at[b], lsend.at[n], lrecv.at[b], to, ep)

    def line_own(n, to):
        return remote(tok, xl.at[z], lsend.at[n], lrecv.at[z], to, ep)

    def line_wait(b):
        line(b, 0, z).wait_recv()

    def icopy(k):
        return remote(idx, idxl.at[z], isend.at[k - 1], irecv.at[z], lax.rem(z + k, NZ), ep)

    @pl.when(inner)
    def _():
        line_own(0, far1).start()

    line_own(1, near).start()
    for k in range(1, NZ):
        icopy(k).start()
    idxl[z] = idx[...]
    xl[z] = tok[...]

    upper = jnp.where(iota((T, T), 0) < iota((T, T), 1), 1.0, 0.0).astype(BF)

    def codes(ids, first, n):
        eid = iota((n, T), 0) + first
        hit = jnp.zeros((n, T), F32)
        for j in range(6):
            hit = hit + jnp.where(ids[j : j + 1, :] == eid, 1.0, 0.0)
        rank = jnp.dot(hit.astype(BF), upper, preferred_element_type=F32)
        return jnp.where(hit > 0.5, rank, -1.0).astype(BF)

    def s_copy(b, k):
        d = lax.rem(ep + k, NE)
        return remote(sel.at[b, d], xr.at[b * NE + ep], ssend.at[b, k - 1], srecv.at[b * NE + ep], z, d)

    def select(b):
        code = codes(idxl[b], z * NE * LE, NE * LE)
        r = iota((PLANE, NE * LE), 0)
        ex = jnp.where(div_cap(r) == iota((PLANE, NE * LE), 1), 1.0, 0.0).astype(BF)
        code_r = jnp.dot(ex, code, preferred_element_type=F32)
        r = iota((PLANE, T), 0)
        slot = (r - div_cap(r) * CAP).astype(F32)
        pick = jnp.where(code_r == slot, 1.0, 0.0).astype(BF)

        def cols(c, _):
            cs = pl.ds(pl.multiple_of(c * DC, DC), DC)
            rows = jnp.dot(pick, xl[b, :, cs], preferred_element_type=F32).astype(BF)
            sel[b, :, :, cs] = rows.reshape(NE, BLK, DC)
            return 0

        lax.fori_loop(0, n_d, cols, 0)
        for k in range(1, NE):
            s_copy(b, k).start()
        xr[b * NE + ep] = sel[b, ep]

    def idx_wait(b):
        remote(idx, idxl.at[b], isend.at[0], irecv.at[b], z, ep).wait_recv()

    select(z)

    n_exp = NDEV * LE
    idx_v, gates_v = idx[...], gates[...]
    code = codes(idx_v, 0, n_exp)
    eid = iota((n_exp, T), 0)
    gate = jnp.zeros((n_exp, T), F32)
    for j in range(6):
        gate = gate + jnp.where(idx_v[j : j + 1, :] == eid, gates_v[j : j + 1, :], 0.0)
    g_hi = gate.astype(BF)
    rest = gate - g_hi.astype(F32)
    g_mid = rest.astype(BF)
    g_lo = (rest - g_mid.astype(F32)).astype(BF)

    def spread(a, ex):
        return lax.dot_general(a, ex, (((0,), (0,)), ((), ())), preferred_element_type=F32)

    for b in range(NZ):
        c = iota((n_exp, PLANE), 1)
        ex = jnp.where(div_cap(c) + b * NE * LE == iota((n_exp, PLANE), 0), 1.0, 0.0).astype(BF)
        c = iota((T, PLANE), 1)
        slot = (c - div_cap(c) * CAP).astype(F32)
        on = spread(code, ex) == slot
        for q, part in enumerate((g_hi, g_mid, g_lo)):
            gm[q, b] = jnp.where(on, spread(part, ex), 0.0).astype(BF)

    def pick_plane(a, b):
        return jnp.where(inner, a, b)

    q0, q1, q2 = pick_plane(far1, near), pick_plane(far2, far1), pick_plane(near, far2)
    line_wait(q0)

    @pl.when(inner)
    def _():
        line(far1, 2, near).start()
        line_wait(near)
        line(near, 3, far1).start()

    idx_wait(q0)
    select(q0)
    line_wait(q1)

    @pl.when(inner)
    def _():
        line(far2, 4, near).start()

    idx_wait(q1)
    select(q1)

    def last_block():
        @pl.when(edge)
        def _():
            line_wait(q2)

        idx_wait(q2)
        select(q2)

    pl.when(inner)(last_block)

    def rows_wait(b):
        for k in range(1, NE):
            i = b * NE + lax.rem(ep + k, NE)
            remote(xr.at[i], xr.at[i], ssend.at[0, 0], srecv.at[i], z, ep).wait_recv()

    def y_copy(zz, ee, e, desc):
        m = zz * NE + ee
        rows = pl.ds(*piece(e, desc))
        return remote(ys.at[m, rows], yr.at[me, rows], ysend.at[e, m], yrecv.at[e, me], zz, ee)

    def experts(p0, p1, n_pass):
        desc = n_pass == 1
        rows_wait(p0)
        rows_wait(p1)

        def step(i, ring, total, copies, before):
            if before:
                if n_pass == 0:
                    for cp in copies(i):
                        cp.wait()
                else:
                    @pl.when(i < total - ring if desc else i >= ring)
                    def _():
                        for cp in copies(i):
                            cp.wait()
            else:
                nxt = i - ring if desc else i + ring

                @pl.when(nxt >= 0 if desc else nxt < total)
                def _():
                    for cp in copies(nxt):
                        cp.start()

        for e in reversed(range(LE)) if desc else range(LE):
            win = WINDOWS[e]
            for s, p in enumerate((p0, p1)):
                def gather(m, _, s=s, p=p):
                    rows = pl.ds(pl.multiple_of(s * NE * 16 + m * 16, 16), 16)
                    a_buf[rows, :] = xr[p * NE + m, win : win + 16, :]
                    return 0

                lax.fori_loop(0, NE, gather, 0)

            def gate_up(c, _):
                c = n_f - 1 - c if desc else c
                i = e * n_f + c
                slot = lax.rem(i, NG)
                step(i, NG, LE * n_f, gu_copies, True)
                a = a_buf[...]
                g = jnp.dot(a, gu[slot, 0], preferred_element_type=F32)
                u = jnp.dot(a, gu[slot, 1], preferred_element_type=F32)
                h_buf[:, pl.ds(pl.multiple_of(c * FC, FC), FC)] = (jax.nn.silu(g) * u).astype(BF)
                step(i, NG, LE * n_f, gu_copies, False)
                return 0

            lax.fori_loop(0, n_f, gate_up, 0)

            def down_proj(c, _):
                c = n_d - 1 - c if desc else c
                i = e * n_d + c
                slot = lax.rem(i, ND)
                step(i, ND, LE * n_d, d_copies, True)
                y = jnp.dot(h_buf[...], wdb[slot], preferred_element_type=F32).reshape(2, NE, 16, DC)
                cs = pl.ds(pl.multiple_of(c * DC, DC), DC)
                second = (e % 2 == 0) == desc
                for s, p in enumerate((p0, p1)):
                    to = pl.ds(p * NE, NE)
                    if not second:
                        ys[to, win : win + 16, cs] = y[s].astype(BF)
                    elif e % 2:
                        old = ys[to, win : win + 8, cs].astype(F32)
                        keep = iota((NE, 8, DC), 1) < 4
                        ys[to, win : win + 8, cs] = jnp.where(keep, old, y[s, :, :8]).astype(BF)
                        ys[to, win + 8 : win + 16, cs] = y[s, :, 8:].astype(BF)
                    else:
                        old = ys[to, win + 8 : win + 16, cs].astype(F32)
                        keep = iota((NE, 8, DC), 1) >= 4
                        ys[to, win + 8 : win + 16, cs] = jnp.where(keep, old, y[s, :, 8:]).astype(BF)
                        ys[to, win : win + 8, cs] = y[s, :, :8].astype(BF)
                step(i, ND, LE * n_d, d_copies, False)
                return 0

            lax.fori_loop(0, n_d, down_proj, 0)

            for k in range(NE):
                y_copy(p0, k, e, desc).start()
            for k in range(NE):
                @pl.when((p1 != z) | (k != ep))
                def _(k=k):
                    y_copy(p1, k, e, desc).start()
            if n_pass == 0 and e == LE - 2:
                pl.when(edge)(last_block)

    experts(pick_plane(far1, near), pick_plane(far2, z), 0)
    experts(pick_plane(near, far2), pick_plane(z, far1), 1)

    yr[me] = ys[me]

    def y_wait(i, desc):
        for e in range(LE):
            rows = pl.ds(*piece(e, desc))
            remote(yr.at[i, rows], yr.at[i, rows], ysend.at[0, 0], yrecv.at[e, i], z, ep).wait_recv()

    late_in = (inner, edge, z < 0, z >= 0)
    late_out = (inner, inner, edge, edge)

    for n, b in enumerate((z, near, far1, far2)):
        for k in range(1 if n == 0 else 0, NE):
            i = b * NE + (lax.rem(ep + k, NE) if n == 0 else k)

            @pl.when(late_in[n])
            def _(i=i):
                y_wait(i, True)

            @pl.when(jnp.logical_not(late_in[n]))
            def _(i=i):
                y_wait(i, False)

        def mix(c, _):
            cs = pl.ds(pl.multiple_of(c * DC, DC), DC)
            rows = yr[pl.ds(b * NE, NE), :, cs].reshape(PLANE, DC)
            s = tok[:, cs].astype(F32) if n == 0 else acc[:, cs]
            for q in range(3):
                s = s + jnp.dot(gm[q, b], rows, preferred_element_type=F32)
            if n < NZ - 1:
                acc[:, cs] = s
            else:
                out[:, cs] = s.astype(BF)
            return 0

        lax.fori_loop(0, n_d, mix, 0)

    for k in range(1, NZ):
        icopy(k).wait_send()
    for b in range(NZ):
        for k in range(1, NE):
            s_copy(b, k).wait_send()
    line_own(1, near).wait_send()

    @pl.when(inner)
    def _():
        line_own(0, far1).wait_send()
        line(far1, 2, near).wait_send()
        line(near, 3, far1).wait_send()
        line(far2, 4, near).wait_send()

    for n, b in enumerate((z, near, far1, far2)):
        for k in range(1 if n == 0 else 0, NE):
            d = lax.rem(ep + k, NE) if n == 0 else k
            for desc in (False, True):
                @pl.when(late_out[n] if desc else jnp.logical_not(late_out[n]))
                def _(b=b, d=d, desc=desc):
                    for e in range(LE):
                        y_copy(b, d, e, desc).wait_send()


def solution(mesh):
    row_spec = P(('dp', 'ep2', 'ep'), None)
    weight_spec = P(('ep2', 'ep'), None, None)

    def local_step(tokens, expert_idx, gates, w_gate, w_up, w_down):
        T, D = tokens.shape
        F = w_gate.shape[2]
        vm = pl.BlockSpec(memory_space=pltpu.VMEM)
        hbm = pl.BlockSpec(memory_space=pl.ANY)
        dma = pltpu.SemaphoreType.DMA
        return pl.pallas_call(
            kernel,
            name="moe",
            out_shape=jax.ShapeDtypeStruct((T, D), BF),
            in_specs=[vm, vm, vm, hbm, hbm, hbm],
            out_specs=vm,
            scratch_shapes=[
                pltpu.VMEM((NZ, T, D), BF),
                pltpu.VMEM((NZ, 6, T), jnp.int32),
                pltpu.VMEM((NZ, NE, BLK, D), BF),
                pltpu.VMEM((NDEV, BLK, D), BF),
                pltpu.VMEM((2 * NE * 16, D), BF),
                pltpu.VMEM((2 * NE * 16, F), BF),
                pltpu.VMEM((NDEV, BLK, D), BF),
                pltpu.VMEM((NDEV, BLK, D), BF),
                pltpu.VMEM((3, NZ, T, PLANE), BF),
                pltpu.VMEM((T, D), F32),
                pltpu.VMEM((NG, 2, D, FC), BF),
                pltpu.VMEM((ND, F, DC), BF),
                dma((NG, 2)),
                dma((ND,)),
                dma((NZ - 1,)),
                dma((NZ,)),
                dma((5,)),
                dma((NZ,)),
                dma((NZ, NE - 1)),
                dma((NDEV,)),
                dma((LE, NDEV)),
                dma((LE, NDEV)),
            ],
            compiler_params=pltpu.CompilerParams(
                collective_id=0, has_side_effects=True, vmem_limit_bytes=67043328
            ),
        )(tokens, expert_idx.T, gates.T, w_gate, w_up, w_down)

    return jax.shard_map(local_step, mesh=mesh, in_specs=(row_spec, row_spec, row_spec, weight_spec, weight_spec, weight_spec), out_specs=row_spec, check_vma=False)
```

```python
import functools

import jax
import jax.numpy as jnp
from jax import lax
from jax.experimental import pallas as pl
from jax.experimental.pallas import tpu as pltpu
from jax.sharding import PartitionSpec as P

MESH = pl.DeviceIdType.MESH
BF = jnp.bfloat16
F32 = jnp.float32
NZ = 4
NE = 4
NDEV = NZ * NE
LE = 4
CAP = 12
BLK = LE * CAP
PLANE = NE * BLK
HALF = BLK // 2
WINDOWS = (0, 8, 24, 32)
FC = 512
DC = 512
NG = 5
ND = 6
PARTS = 2


def iota(shape, dim):
    return lax.broadcasted_iota(jnp.int32, shape, dim)


def div_cap(v):
    return (v * 43691) >> 19


def piece(e, desc):
    base = (e // 2) * HALF
    if desc:
        return (base + 16, 8) if e % 2 else (base, 16)
    return (base + 8, 16) if e % 2 else (base, 8)


def kernel(tok, idx, gates, wg, wu, wd, out, xl, idxl, sel, xr, a_buf, h_buf, ys, yr, gm, acc, pick, gu, wdb,
           gsem, dsem, isend, irecv, lsend, lrecv, ssend, srecv, ysend, yrecv):
    T, D = tok.shape
    F = wg.shape[2]
    n_f, n_d = F // FC, D // DC
    dp, z, ep = lax.axis_index("dp"), lax.axis_index("ep2"), lax.axis_index("ep")
    me = z * NE + ep
    low = z < NZ // 2
    inner = (z == 1) | (z == 2)
    edge = jnp.logical_not(inner)
    near = jnp.where(low, 1 - z, 5 - z)
    far1 = jnp.where(low, 2, 1)
    far2 = jnp.where(low, 3, 0)

    def remote(src, dst, ss, rs, zz, ee):
        return pltpu.make_async_remote_copy(
            src_ref=src, dst_ref=dst, send_sem=ss, recv_sem=rs, device_id=(dp, zz, ee), device_id_type=MESH
        )

    def gu_copies(i):
        e, c, slot = lax.div(i, n_f), lax.rem(i, n_f), lax.rem(i, NG)
        cols = pl.ds(pl.multiple_of(c * FC, FC), FC)
        return (
            pltpu.make_async_copy(wg.at[e, :, cols], gu.at[slot, 0], gsem.at[slot, 0]),
            pltpu.make_async_copy(wu.at[e, :, cols], gu.at[slot, 1], gsem.at[slot, 1]),
        )

    def d_copies(i):
        e, c, slot = lax.div(i, n_d), lax.rem(i, n_d), lax.rem(i, ND)
        cols = pl.ds(pl.multiple_of(c * DC, DC), DC)
        return (pltpu.make_async_copy(wd.at[e, :, cols], wdb.at[slot], dsem.at[slot]),)

    for i in range(NG):
        for cp in gu_copies(jnp.int32(i)):
            cp.start()
    for i in range(ND):
        for cp in d_copies(jnp.int32(i)):
            cp.start()

    barrier = pltpu.get_barrier_semaphore()
    for k in range(1, NDEV):
        peer = lax.rem(me + k, NDEV)
        pl.semaphore_signal(barrier, inc=1, device_id=(dp, lax.div(peer, NE), lax.rem(peer, NE)), device_id_type=MESH)
    pl.semaphore_wait(barrier, NDEV - 1)

    def span(h):
        return pl.ds(h * (D // PARTS), D // PARTS)

    def line(b, n, to, h):
        at = xl.at[b, :, span(h)]
        return remote(at, at, lsend.at[n, h], lrecv.at[b, h], to, ep)

    def line_own(n, to, h):
        return remote(tok.at[:, span(h)], xl.at[z, :, span(h)], lsend.at[n, h], lrecv.at[z, h], to, ep)

    def line_wait(b, h):
        line(b, 0, z, h).wait_recv()

    def icopy(k):
        return remote(idx, idxl.at[z], isend.at[k - 1], irecv.at[z], lax.rem(z + k, NZ), ep)

    for h in range(PARTS):
        @pl.when(inner)
        def _(h=h):
            line_own(0, far1, h).start()

        line_own(1, near, h).start()
    for k in range(1, NZ):
        icopy(k).start()
    idxl[z] = idx[...]
    xl[z] = tok[...]

    upper = jnp.where(iota((T, T), 0) < iota((T, T), 1), 1.0, 0.0).astype(BF)

    def codes(ids, first, n):
        eid = iota((n, T), 0) + first
        hit = jnp.zeros((n, T), F32)
        for j in range(6):
            hit = hit + jnp.where(ids[j : j + 1, :] == eid, 1.0, 0.0)
        rank = jnp.dot(hit.astype(BF), upper, preferred_element_type=F32)
        return jnp.where(hit > 0.5, rank, -1.0).astype(BF)

    def s_copy(b, k, h):
        d = lax.rem(ep + k, NE)
        return remote(
            sel.at[b, d, :, span(h)], xr.at[b * NE + ep, :, span(h)], ssend.at[b, k - 1, h],
            srecv.at[b * NE + ep, h], z, d
        )

    def picks(b):
        code = codes(idxl[b], z * NE * LE, NE * LE)
        r = iota((PLANE, NE * LE), 0)
        ex = jnp.where(div_cap(r) == iota((PLANE, NE * LE), 1), 1.0, 0.0).astype(BF)
        code_r = jnp.dot(ex, code, preferred_element_type=F32)
        r = iota((PLANE, T), 0)
        slot = (r - div_cap(r) * CAP).astype(F32)
        pick[...] = jnp.where(code_r == slot, 1.0, 0.0).astype(BF)

    def select(b, h):
        wide = D // PARTS // 2

        def cols(c, _):
            cs = pl.ds(pl.multiple_of(h * (D // PARTS) + c * wide, 128), wide)
            rows = jnp.dot(pick[...], xl[b, :, cs], preferred_element_type=F32).astype(BF)
            sel[b, :, :, cs] = rows.reshape(NE, BLK, wide)
            return 0

        lax.fori_loop(0, 2, cols, 0)
        for k in range(1, NE):
            s_copy(b, k, h).start()
        xr[b * NE + ep, :, span(h)] = sel[b, ep, :, span(h)]

    def idx_wait(b):
        remote(idx, idxl.at[b], isend.at[0], irecv.at[b], z, ep).wait_recv()

    picks(z)
    for h in range(PARTS):
        select(z, h)

    n_exp = NDEV * LE
    idx_v, gates_v = idx[...], gates[...]
    code = codes(idx_v, 0, n_exp)
    eid = iota((n_exp, T), 0)
    gate = jnp.zeros((n_exp, T), F32)
    for j in range(6):
        gate = gate + jnp.where(idx_v[j : j + 1, :] == eid, gates_v[j : j + 1, :], 0.0)
    g_hi = gate.astype(BF)
    rest = gate - g_hi.astype(F32)
    g_mid = rest.astype(BF)
    g_lo = (rest - g_mid.astype(F32)).astype(BF)

    def spread(a, ex):
        return lax.dot_general(a, ex, (((0,), (0,)), ((), ())), preferred_element_type=F32)

    for b in range(NZ):
        c = iota((n_exp, PLANE), 1)
        ex = jnp.where(div_cap(c) + b * NE * LE == iota((n_exp, PLANE), 0), 1.0, 0.0).astype(BF)
        c = iota((T, PLANE), 1)
        slot = (c - div_cap(c) * CAP).astype(F32)
        on = spread(code, ex) == slot
        for q, part in enumerate((g_hi, g_mid, g_lo)):
            gm[q, b] = jnp.where(on, spread(part, ex), 0.0).astype(BF)

    def pick_plane(a, b):
        return jnp.where(inner, a, b)

    q0, q1, q2 = pick_plane(far1, near), pick_plane(far2, far1), pick_plane(near, far2)
    for h in range(PARTS):
        line_wait(q0, h)

        @pl.when(inner)
        def _(h=h):
            line(far1, 2, near, h).start()
            line_wait(near, h)
            line(near, 3, far1, h).start()

        if h == 0:
            idx_wait(q0)
            picks(q0)
        select(q0, h)

    for h in range(PARTS):
        if h == 0:
            idx_wait(q1)
            picks(q1)
        line_wait(q1, h)

        @pl.when(inner)
        def _(h=h):
            line(far2, 4, near, h).start()

        select(q1, h)

    def last_block():
        idx_wait(q2)
        picks(q2)
        for h in range(PARTS):
            @pl.when(edge)
            def _(h=h):
                line_wait(q2, h)

            select(q2, h)

    pl.when(inner)(last_block)

    def rows_wait(b):
        for k in range(1, NE):
            i = b * NE + lax.rem(ep + k, NE)
            for h in range(PARTS):
                at = xr.at[i, :, span(h)]
                remote(at, at, ssend.at[0, 0, 0], srecv.at[i, h], z, ep).wait_recv()

    def y_copy(zz, ee, e, desc):
        m = zz * NE + ee
        rows = pl.ds(*piece(e, desc))
        return remote(ys.at[m, rows], yr.at[me, rows], ysend.at[e, m], yrecv.at[e, me], zz, ee)

    def experts(p0, p1, n_pass):
        desc = n_pass == 1
        rows_wait(p0)
        rows_wait(p1)

        def step(i, ring, total, copies, before):
            if before:
                if n_pass == 0:
                    for cp in copies(i):
                        cp.wait()
                else:
                    @pl.when(i < total - ring if desc else i >= ring)
                    def _():
                        for cp in copies(i):
                            cp.wait()
            else:
                nxt = i - ring if desc else i + ring

                @pl.when(nxt >= 0 if desc else nxt < total)
                def _():
                    for cp in copies(nxt):
                        cp.start()

        for e in reversed(range(LE)) if desc else range(LE):
            win = WINDOWS[e]
            for s, p in enumerate((p0, p1)):
                def gather(m, _, s=s, p=p):
                    rows = pl.ds(pl.multiple_of(s * NE * 16 + m * 16, 16), 16)
                    a_buf[rows, :] = xr[p * NE + m, win : win + 16, :]
                    return 0

                lax.fori_loop(0, NE, gather, 0)

            def gate_up(c, _):
                c = n_f - 1 - c if desc else c
                i = e * n_f + c
                slot = lax.rem(i, NG)
                step(i, NG, LE * n_f, gu_copies, True)
                a = a_buf[...]
                g = jnp.dot(a, gu[slot, 0], preferred_element_type=F32)
                u = jnp.dot(a, gu[slot, 1], preferred_element_type=F32)
                h_buf[:, pl.ds(pl.multiple_of(c * FC, FC), FC)] = (jax.nn.silu(g) * u).astype(BF)
                step(i, NG, LE * n_f, gu_copies, False)
                return 0

            lax.fori_loop(0, n_f, gate_up, 0)

            def down_proj(c, _):
                c = n_d - 1 - c if desc else c
                i = e * n_d + c
                slot = lax.rem(i, ND)
                step(i, ND, LE * n_d, d_copies, True)
                y = jnp.dot(h_buf[...], wdb[slot], preferred_element_type=F32).reshape(2, NE, 16, DC)
                cs = pl.ds(pl.multiple_of(c * DC, DC), DC)
                second = (e % 2 == 0) == desc
                for s, p in enumerate((p0, p1)):
                    to = pl.ds(p * NE, NE)
                    if not second:
                        ys[to, win : win + 16, cs] = y[s].astype(BF)
                    elif e % 2:
                        old = ys[to, win : win + 8, cs].astype(F32)
                        keep = iota((NE, 8, DC), 1) < 4
                        ys[to, win : win + 8, cs] = jnp.where(keep, old, y[s, :, :8]).astype(BF)
                        ys[to, win + 8 : win + 16, cs] = y[s, :, 8:].astype(BF)
                    else:
                        old = ys[to, win + 8 : win + 16, cs].astype(F32)
                        keep = iota((NE, 8, DC), 1) >= 4
                        ys[to, win + 8 : win + 16, cs] = jnp.where(keep, old, y[s, :, 8:]).astype(BF)
                        ys[to, win : win + 8, cs] = y[s, :, :8].astype(BF)
                step(i, ND, LE * n_d, d_copies, False)
                return 0

            lax.fori_loop(0, n_d, down_proj, 0)

            for k in range(NE):
                y_copy(p0, k, e, desc).start()
            for k in range(NE):
                @pl.when((p1 != z) | (k != ep))
                def _(k=k):
                    y_copy(p1, k, e, desc).start()
            if n_pass == 0 and e == LE - 2:
                pl.when(edge)(last_block)

    experts(pick_plane(far1, near), pick_plane(far2, z), 0)
    experts(pick_plane(near, far2), pick_plane(z, far1), 1)

    yr[me] = ys[me]

    def y_wait(i, desc):
        for e in range(LE):
            rows = pl.ds(*piece(e, desc))
            remote(yr.at[i, rows], yr.at[i, rows], ysend.at[0, 0], yrecv.at[e, i], z, ep).wait_recv()

    late_in = (inner, edge, z < 0, z >= 0)
    late_out = (inner, inner, edge, edge)

    for n, b in enumerate((z, near, far1, far2)):
        for k in range(1 if n == 0 else 0, NE):
            i = b * NE + (lax.rem(ep + k, NE) if n == 0 else k)

            @pl.when(late_in[n])
            def _(i=i):
                y_wait(i, True)

            @pl.when(jnp.logical_not(late_in[n]))
            def _(i=i):
                y_wait(i, False)

        def mix(c, _):
            cs = pl.ds(pl.multiple_of(c * DC, DC), DC)
            rows = yr[pl.ds(b * NE, NE), :, cs].reshape(PLANE, DC)
            s = tok[:, cs].astype(F32) if n == 0 else acc[:, cs]
            for q in range(3):
                s = s + jnp.dot(gm[q, b], rows, preferred_element_type=F32)
            if n < NZ - 1:
                acc[:, cs] = s
            else:
                out[:, cs] = s.astype(BF)
            return 0

        lax.fori_loop(0, n_d, mix, 0)

    for k in range(1, NZ):
        icopy(k).wait_send()
    for b in range(NZ):
        for k in range(1, NE):
            for h in range(PARTS):
                s_copy(b, k, h).wait_send()
    for h in range(PARTS):
        line_own(1, near, h).wait_send()

        @pl.when(inner)
        def _(h=h):
            line_own(0, far1, h).wait_send()
            line(far1, 2, near, h).wait_send()
            line(near, 3, far1, h).wait_send()
            line(far2, 4, near, h).wait_send()

    for n, b in enumerate((z, near, far1, far2)):
        for k in range(1 if n == 0 else 0, NE):
            d = lax.rem(ep + k, NE) if n == 0 else k
            for desc in (False, True):
                @pl.when(late_out[n] if desc else jnp.logical_not(late_out[n]))
                def _(b=b, d=d, desc=desc):
                    for e in range(LE):
                        y_copy(b, d, e, desc).wait_send()


def solution(mesh):
    row_spec = P(('dp', 'ep2', 'ep'), None)
    weight_spec = P(('ep2', 'ep'), None, None)

    def local_step(tokens, expert_idx, gates, w_gate, w_up, w_down):
        T, D = tokens.shape
        F = w_gate.shape[2]
        vm = pl.BlockSpec(memory_space=pltpu.VMEM)
        hbm = pl.BlockSpec(memory_space=pl.ANY)
        dma = pltpu.SemaphoreType.DMA
        return pl.pallas_call(
            kernel,
            name="moe",
            out_shape=jax.ShapeDtypeStruct((T, D), BF),
            in_specs=[vm, vm, vm, hbm, hbm, hbm],
            out_specs=vm,
            scratch_shapes=[
                pltpu.VMEM((NZ, T, D), BF),
                pltpu.VMEM((NZ, 6, T), jnp.int32),
                pltpu.VMEM((NZ, NE, BLK, D), BF),
                pltpu.VMEM((NDEV, BLK, D), BF),
                pltpu.VMEM((2 * NE * 16, D), BF),
                pltpu.VMEM((2 * NE * 16, F), BF),
                pltpu.VMEM((NDEV, BLK, D), BF),
                pltpu.VMEM((NDEV, BLK, D), BF),
                pltpu.VMEM((3, NZ, T, PLANE), BF),
                pltpu.VMEM((T, D), F32),
                pltpu.VMEM((PLANE, T), BF),
                pltpu.VMEM((NG, 2, D, FC), BF),
                pltpu.VMEM((ND, F, DC), BF),
                dma((NG, 2)),
                dma((ND,)),
                dma((NZ - 1,)),
                dma((NZ,)),
                dma((5, PARTS)),
                dma((NZ, PARTS)),
                dma((NZ, NE - 1, PARTS)),
                dma((NDEV, PARTS)),
                dma((LE, NDEV)),
                dma((LE, NDEV)),
            ],
            compiler_params=pltpu.CompilerParams(
                collective_id=0, has_side_effects=True, vmem_limit_bytes=67043328
            ),
        )(tokens, expert_idx.T, gates.T, w_gate, w_up, w_down)

    return jax.shard_map(local_step, mesh=mesh, in_specs=(row_spec, row_spec, row_spec, weight_spec, weight_spec, weight_spec), out_specs=row_spec, check_vma=False)
```

```python
import functools

import jax
import jax.numpy as jnp
from jax import lax
from jax.experimental import pallas as pl
from jax.experimental.pallas import tpu as pltpu
from jax.sharding import PartitionSpec as P

MESH = pl.DeviceIdType.MESH
BF = jnp.bfloat16
F32 = jnp.float32
NZ = 4
NE = 4
NDEV = NZ * NE
LE = 4
CAP = 12
BLK = LE * CAP
PLANE = NE * BLK
HALF = BLK // 2
WINDOWS = (0, 8, 24, 32)
FC = 512
DC = 512
NG = 5
ND = 6
PARTS = 2


def iota(shape, dim):
    return lax.broadcasted_iota(jnp.int32, shape, dim)


def div_cap(v):
    return (v * 43691) >> 19


def piece(e, desc):
    base = (e // 2) * HALF
    if desc:
        return (base + 16, 8) if e % 2 else (base, 16)
    return (base + 8, 16) if e % 2 else (base, 8)


def kernel(tok, idx, gates, wg, wu, wd, out, xl, idxl, sel, xr, a_buf, h_buf, ys, yr, gm, acc, pick, gu, wdb,
           gsem, dsem, isend, irecv, lsend, lrecv, ssend, srecv, ysend, yrecv):
    T, D = tok.shape
    F = wg.shape[2]
    n_f, n_d = F // FC, D // DC
    dp, z, ep = lax.axis_index("dp"), lax.axis_index("ep2"), lax.axis_index("ep")
    me = z * NE + ep
    low = z < NZ // 2
    inner = (z == 1) | (z == 2)
    edge = jnp.logical_not(inner)
    near = jnp.where(low, 1 - z, 5 - z)
    far1 = jnp.where(low, 2, 1)
    far2 = jnp.where(low, 3, 0)

    def remote(src, dst, ss, rs, zz, ee):
        return pltpu.make_async_remote_copy(
            src_ref=src, dst_ref=dst, send_sem=ss, recv_sem=rs, device_id=(dp, zz, ee), device_id_type=MESH
        )

    def gu_copies(i):
        e, c, slot = lax.div(i, n_f), lax.rem(i, n_f), lax.rem(i, NG)
        cols = pl.ds(pl.multiple_of(c * FC, FC), FC)
        return (
            pltpu.make_async_copy(wg.at[e, :, cols], gu.at[slot, 0], gsem.at[slot, 0]),
            pltpu.make_async_copy(wu.at[e, :, cols], gu.at[slot, 1], gsem.at[slot, 1]),
        )

    def d_copies(i):
        e, c, slot = lax.div(i, n_d), lax.rem(i, n_d), lax.rem(i, ND)
        cols = pl.ds(pl.multiple_of(c * DC, DC), DC)
        return (pltpu.make_async_copy(wd.at[e, :, cols], wdb.at[slot], dsem.at[slot]),)

    for i in range(NG):
        for cp in gu_copies(jnp.int32(i)):
            cp.start()
    for i in range(ND):
        for cp in d_copies(jnp.int32(i)):
            cp.start()

    barrier = pltpu.get_barrier_semaphore()
    for k in range(1, NDEV):
        peer = lax.rem(me + k, NDEV)
        pl.semaphore_signal(barrier, inc=1, device_id=(dp, lax.div(peer, NE), lax.rem(peer, NE)), device_id_type=MESH)
    pl.semaphore_wait(barrier, NDEV - 1)

    def span(h):
        return pl.ds(h * (D // PARTS), D // PARTS)

    def line(b, n, to, h):
        at = xl.at[b, :, span(h)]
        return remote(at, at, lsend.at[n, h], lrecv.at[b, h], to, ep)

    def line_own(n, to, h):
        return remote(tok.at[:, span(h)], xl.at[z, :, span(h)], lsend.at[n, h], lrecv.at[z, h], to, ep)

    def line_wait(b, h):
        line(b, 0, z, h).wait_recv()

    def icopy(k):
        return remote(idx, idxl.at[z], isend.at[k - 1], irecv.at[z], lax.rem(z + k, NZ), ep)

    for h in range(PARTS):
        @pl.when(inner)
        def _(h=h):
            line_own(0, far1, h).start()

        line_own(1, near, h).start()
    for k in range(1, NZ):
        icopy(k).start()
    idxl[z] = idx[...]
    xl[z] = tok[...]

    upper = jnp.where(iota((T, T), 0) < iota((T, T), 1), 1.0, 0.0).astype(BF)

    def codes(ids, first, n):
        eid = iota((n, T), 0) + first
        hit = jnp.zeros((n, T), F32)
        for j in range(6):
            hit = hit + jnp.where(ids[j : j + 1, :] == eid, 1.0, 0.0)
        rank = jnp.dot(hit.astype(BF), upper, preferred_element_type=F32)
        return jnp.where(hit > 0.5, rank, -1.0).astype(BF)

    def s_copy(b, k, h):
        d = lax.rem(ep + k, NE)
        return remote(
            sel.at[b, d, :, span(h)], xr.at[b * NE + ep, :, span(h)], ssend.at[b, k - 1, h],
            srecv.at[b * NE + ep, h], z, d
        )

    def picks(b):
        code = codes(idxl[b], z * NE * LE, NE * LE)
        r = iota((PLANE, NE * LE), 0)
        ex = jnp.where(div_cap(r) == iota((PLANE, NE * LE), 1), 1.0, 0.0).astype(BF)
        code_r = jnp.dot(ex, code, preferred_element_type=F32)
        r = iota((PLANE, T), 0)
        slot = (r - div_cap(r) * CAP).astype(F32)
        pick[...] = jnp.where(code_r == slot, 1.0, 0.0).astype(BF)

    def select(b, h):
        wide = D // PARTS // 2

        def cols(c, _):
            cs = pl.ds(pl.multiple_of(h * (D // PARTS) + c * wide, 128), wide)
            rows = jnp.dot(pick[...], xl[b, :, cs], preferred_element_type=F32).astype(BF)
            sel[b, :, :, cs] = rows.reshape(NE, BLK, wide)
            return 0

        lax.fori_loop(0, 2, cols, 0)
        for k in range(1, NE):
            s_copy(b, k, h).start()
        xr[b * NE + ep, :, span(h)] = sel[b, ep, :, span(h)]

    def idx_wait(b):
        remote(idx, idxl.at[b], isend.at[0], irecv.at[b], z, ep).wait_recv()

    picks(z)
    for h in range(PARTS):
        select(z, h)

    n_exp = NDEV * LE
    idx_v, gates_v = idx[...], gates[...]
    code = codes(idx_v, 0, n_exp)
    eid = iota((n_exp, T), 0)
    gate = jnp.zeros((n_exp, T), F32)
    for j in range(6):
        gate = gate + jnp.where(idx_v[j : j + 1, :] == eid, gates_v[j : j + 1, :], 0.0)
    g_hi = gate.astype(BF)
    rest = gate - g_hi.astype(F32)
    g_mid = rest.astype(BF)
    g_lo = (rest - g_mid.astype(F32)).astype(BF)

    def spread(a, ex):
        return lax.dot_general(a, ex, (((0,), (0,)), ((), ())), preferred_element_type=F32)

    for b in range(NZ):
        c = iota((n_exp, PLANE), 1)
        ex = jnp.where(div_cap(c) + b * NE * LE == iota((n_exp, PLANE), 0), 1.0, 0.0).astype(BF)
        c = iota((T, PLANE), 1)
        slot = (c - div_cap(c) * CAP).astype(F32)
        on = spread(code, ex) == slot
        for q, part in enumerate((g_hi, g_mid, g_lo)):
            gm[q, b] = jnp.where(on, spread(part, ex), 0.0).astype(BF)

    def pick_plane(a, b):
        return jnp.where(inner, a, b)

    q0, q1, q2 = pick_plane(far1, near), pick_plane(far2, far1), pick_plane(near, far2)
    for h in range(PARTS):
        line_wait(q0, h)

        @pl.when(inner)
        def _(h=h):
            line(far1, 2, near, h).start()
            line_wait(near, h)
            line(near, 3, far1, h).start()

        if h == 0:
            idx_wait(q0)
            picks(q0)
        select(q0, h)

    for h in range(PARTS):
        if h == 0:
            idx_wait(q1)
            picks(q1)
        line_wait(q1, h)

        @pl.when(inner)
        def _(h=h):
            line(far2, 4, near, h).start()

        select(q1, h)

    def last_block():
        idx_wait(q2)
        picks(q2)
        for h in range(PARTS):
            @pl.when(edge)
            def _(h=h):
                line_wait(q2, h)

            select(q2, h)

    pl.when(inner)(last_block)

    def rows_wait(b):
        for k in range(1, NE):
            i = b * NE + lax.rem(ep + k, NE)
            for h in range(PARTS):
                at = xr.at[i, :, span(h)]
                remote(at, at, ssend.at[0, 0, 0], srecv.at[i, h], z, ep).wait_recv()

    def y_copy(zz, ee, e, desc):
        m = zz * NE + ee
        rows = pl.ds(*piece(e, desc))
        return remote(ys.at[m, rows], yr.at[me, rows], ysend.at[e, m], yrecv.at[e, me], zz, ee)

    def experts(p0, p1, n_pass):
        desc = n_pass == 1
        rows_wait(p0)
        rows_wait(p1)

        def step(i, ring, total, copies, before):
            if before:
                if n_pass == 0:
                    for cp in copies(i):
                        cp.wait()
                else:
                    @pl.when(i < total - ring if desc else i >= ring)
                    def _():
                        for cp in copies(i):
                            cp.wait()
            else:
                nxt = i - ring if desc else i + ring

                @pl.when(nxt >= 0 if desc else nxt < total)
                def _():
                    for cp in copies(nxt):
                        cp.start()

        for e in reversed(range(LE)) if desc else range(LE):
            win = WINDOWS[e]
            for s, p in enumerate((p0, p1)):
                def gather(m, _, s=s, p=p):
                    rows = pl.ds(pl.multiple_of(s * NE * 16 + m * 16, 16), 16)
                    a_buf[rows, :] = xr[p * NE + m, win : win + 16, :]
                    return 0

                lax.fori_loop(0, NE, gather, 0)

            def gate_up(c, _):
                c = n_f - 1 - c if desc else c
                i = e * n_f + c
                slot = lax.rem(i, NG)
                step(i, NG, LE * n_f, gu_copies, True)
                a = a_buf[...]
                g = jnp.dot(a, gu[slot, 0], preferred_element_type=F32)
                u = jnp.dot(a, gu[slot, 1], preferred_element_type=F32)
                h_buf[:, pl.ds(pl.multiple_of(c * FC, FC), FC)] = (jax.nn.silu(g) * u).astype(BF)
                step(i, NG, LE * n_f, gu_copies, False)
                return 0

            lax.fori_loop(0, n_f, gate_up, 0)

            def down_proj(c, _):
                c = n_d - 1 - c if desc else c
                i = e * n_d + c
                slot = lax.rem(i, ND)
                step(i, ND, LE * n_d, d_copies, True)
                y = jnp.dot(h_buf[...], wdb[slot], preferred_element_type=F32).reshape(2, NE, 16, DC)
                cs = pl.ds(pl.multiple_of(c * DC, DC), DC)
                second = (e % 2 == 0) == desc
                for s, p in enumerate((p0, p1)):
                    to = pl.ds(p * NE, NE)
                    if not second:
                        ys[to, win : win + 16, cs] = y[s].astype(BF)
                    elif e % 2:
                        old = ys[to, win : win + 8, cs].astype(F32)
                        keep = iota((NE, 8, DC), 1) < 4
                        ys[to, win : win + 8, cs] = jnp.where(keep, old, y[s, :, :8]).astype(BF)
                        ys[to, win + 8 : win + 16, cs] = y[s, :, 8:].astype(BF)
                    else:
                        old = ys[to, win + 8 : win + 16, cs].astype(F32)
                        keep = iota((NE, 8, DC), 1) >= 4
                        ys[to, win + 8 : win + 16, cs] = jnp.where(keep, old, y[s, :, 8:]).astype(BF)
                        ys[to, win : win + 8, cs] = y[s, :, :8].astype(BF)
                step(i, ND, LE * n_d, d_copies, False)
                return 0

            lax.fori_loop(0, n_d, down_proj, 0)

            for k in range(NE):
                y_copy(p0, k, e, desc).start()
            if n_pass:
                for k in range(NE):
                    y_copy(p1, k, e, desc).start()
            elif e == LE - 2:
                pl.when(edge)(last_block)
        if n_pass == 0:
            for e in range(LE):
                for k in range(1, NE):
                    y_copy(z, lax.rem(ep + k, NE), e, desc).start()

    experts(pick_plane(far1, near), z, 0)
    experts(far2, pick_plane(near, far1), 1)

    yr[me] = ys[me]

    def y_wait(i, desc):
        for e in range(LE):
            rows = pl.ds(*piece(e, desc))
            remote(yr.at[i, rows], yr.at[i, rows], ysend.at[0, 0], yrecv.at[e, i], z, ep).wait_recv()

    late_in = (z < 0, edge, edge, z >= 0)
    late_out = (z < 0, inner, edge, z >= 0)

    for n, b in enumerate((z, near, far1, far2)):
        for k in range(1 if n == 0 else 0, NE):
            i = b * NE + (lax.rem(ep + k, NE) if n == 0 else k)

            @pl.when(late_in[n])
            def _(i=i):
                y_wait(i, True)

            @pl.when(jnp.logical_not(late_in[n]))
            def _(i=i):
                y_wait(i, False)

        def mix(c, _):
            cs = pl.ds(pl.multiple_of(c * DC, DC), DC)
            rows = yr[pl.ds(b * NE, NE), :, cs].reshape(PLANE, DC)
            s = tok[:, cs].astype(F32) if n == 0 else acc[:, cs]
            for q in range(3):
                s = s + jnp.dot(gm[q, b], rows, preferred_element_type=F32)
            if n < NZ - 1:
                acc[:, cs] = s
            else:
                out[:, cs] = s.astype(BF)
            return 0

        lax.fori_loop(0, n_d, mix, 0)

    for k in range(1, NZ):
        icopy(k).wait_send()
    for b in range(NZ):
        for k in range(1, NE):
            for h in range(PARTS):
                s_copy(b, k, h).wait_send()
    for h in range(PARTS):
        line_own(1, near, h).wait_send()

        @pl.when(inner)
        def _(h=h):
            line_own(0, far1, h).wait_send()
            line(far1, 2, near, h).wait_send()
            line(near, 3, far1, h).wait_send()
            line(far2, 4, near, h).wait_send()

    for n, b in enumerate((z, near, far1, far2)):
        for k in range(1 if n == 0 else 0, NE):
            d = lax.rem(ep + k, NE) if n == 0 else k
            for desc in (False, True):
                @pl.when(late_out[n] if desc else jnp.logical_not(late_out[n]))
                def _(b=b, d=d, desc=desc):
                    for e in range(LE):
                        y_copy(b, d, e, desc).wait_send()


def solution(mesh):
    row_spec = P(('dp', 'ep2', 'ep'), None)
    weight_spec = P(('ep2', 'ep'), None, None)

    def local_step(tokens, expert_idx, gates, w_gate, w_up, w_down):
        T, D = tokens.shape
        F = w_gate.shape[2]
        vm = pl.BlockSpec(memory_space=pltpu.VMEM)
        hbm = pl.BlockSpec(memory_space=pl.ANY)
        dma = pltpu.SemaphoreType.DMA
        return pl.pallas_call(
            kernel,
            name="moe",
            out_shape=jax.ShapeDtypeStruct((T, D), BF),
            in_specs=[vm, vm, vm, hbm, hbm, hbm],
            out_specs=vm,
            scratch_shapes=[
                pltpu.VMEM((NZ, T, D), BF),
                pltpu.VMEM((NZ, 6, T), jnp.int32),
                pltpu.VMEM((NZ, NE, BLK, D), BF),
                pltpu.VMEM((NDEV, BLK, D), BF),
                pltpu.VMEM((2 * NE * 16, D), BF),
                pltpu.VMEM((2 * NE * 16, F), BF),
                pltpu.VMEM((NDEV, BLK, D), BF),
                pltpu.VMEM((NDEV, BLK, D), BF),
                pltpu.VMEM((3, NZ, T, PLANE), BF),
                pltpu.VMEM((T, D), F32),
                pltpu.VMEM((PLANE, T), BF),
                pltpu.VMEM((NG, 2, D, FC), BF),
                pltpu.VMEM((ND, F, DC), BF),
                dma((NG, 2)),
                dma((ND,)),
                dma((NZ - 1,)),
                dma((NZ,)),
                dma((5, PARTS)),
                dma((NZ, PARTS)),
                dma((NZ, NE - 1, PARTS)),
                dma((NDEV, PARTS)),
                dma((LE, NDEV)),
                dma((LE, NDEV)),
            ],
            compiler_params=pltpu.CompilerParams(
                collective_id=0, has_side_effects=True, vmem_limit_bytes=67043328
            ),
        )(tokens, expert_idx.T, gates.T, w_gate, w_up, w_down)

    return jax.shard_map(local_step, mesh=mesh, in_specs=(row_spec, row_spec, row_spec, weight_spec, weight_spec, weight_spec), out_specs=row_spec, check_vma=False)
```

```python
import functools

import jax
import jax.numpy as jnp
from jax import lax
from jax.experimental import pallas as pl
from jax.experimental.pallas import tpu as pltpu
from jax.sharding import PartitionSpec as P

MESH = pl.DeviceIdType.MESH
BF = jnp.bfloat16
F32 = jnp.float32
NZ = 4
NE = 4
NDEV = NZ * NE
LE = 4
CAP = 12
BLK = LE * CAP
PLANE = NE * BLK
HALF = BLK // 2
WINDOWS = (0, 8, 24, 32)
FC = 512
DC = 512
NG = 5
ND = 6
PARTS = 2


def iota(shape, dim):
    return lax.broadcasted_iota(jnp.int32, shape, dim)


def div_cap(v):
    return (v * 43691) >> 19


def piece(e, desc):
    base = (e // 2) * HALF
    if desc:
        return (base + 16, 8) if e % 2 else (base, 16)
    return (base + 8, 16) if e % 2 else (base, 8)


def kernel(tok, idx, gates, wg, wu, wd, out, xl, idxl, sel, xr, a_buf, h_buf, ys, yr, gm, acc, pick, gu, wdb,
           gsem, dsem, isend, irecv, lsend, lrecv, ssend, srecv, ysend, yrecv):
    T, D = tok.shape
    F = wg.shape[2]
    n_f, n_d = F // FC, D // DC
    dp, z, ep = lax.axis_index("dp"), lax.axis_index("ep2"), lax.axis_index("ep")
    me = z * NE + ep
    low = z < NZ // 2
    inner = (z == 1) | (z == 2)
    edge = jnp.logical_not(inner)
    near = jnp.where(low, 1 - z, 5 - z)
    far1 = jnp.where(low, 2, 1)
    far2 = jnp.where(low, 3, 0)

    def remote(src, dst, ss, rs, zz, ee):
        return pltpu.make_async_remote_copy(
            src_ref=src, dst_ref=dst, send_sem=ss, recv_sem=rs, device_id=(dp, zz, ee), device_id_type=MESH
        )

    def gu_copies(i):
        e, c, slot = lax.div(i, n_f), lax.rem(i, n_f), lax.rem(i, NG)
        cols = pl.ds(pl.multiple_of(c * FC, FC), FC)
        return (
            pltpu.make_async_copy(wg.at[e, :, cols], gu.at[slot, 0], gsem.at[slot, 0]),
            pltpu.make_async_copy(wu.at[e, :, cols], gu.at[slot, 1], gsem.at[slot, 1]),
        )

    def d_copies(i):
        e, c, slot = lax.div(i, n_d), lax.rem(i, n_d), lax.rem(i, ND)
        cols = pl.ds(pl.multiple_of(c * DC, DC), DC)
        return (pltpu.make_async_copy(wd.at[e, :, cols], wdb.at[slot], dsem.at[slot]),)

    for i in range(NG):
        for cp in gu_copies(jnp.int32(i)):
            cp.start()
    for i in range(ND):
        for cp in d_copies(jnp.int32(i)):
            cp.start()

    barrier = pltpu.get_barrier_semaphore()
    for k in range(1, NDEV):
        peer = lax.rem(me + k, NDEV)
        pl.semaphore_signal(barrier, inc=1, device_id=(dp, lax.div(peer, NE), lax.rem(peer, NE)), device_id_type=MESH)
    pl.semaphore_wait(barrier, NDEV - 1)

    def span(h):
        return pl.ds(h * (D // PARTS), D // PARTS)

    def line(b, n, to, h):
        at = xl.at[b, :, span(h)]
        return remote(at, at, lsend.at[n, h], lrecv.at[b, h], to, ep)

    def line_own(n, to, h):
        return remote(tok.at[:, span(h)], xl.at[z, :, span(h)], lsend.at[n, h], lrecv.at[z, h], to, ep)

    def line_wait(b, h):
        line(b, 0, z, h).wait_recv()

    def icopy(k):
        return remote(idx, idxl.at[z], isend.at[k - 1], irecv.at[z], lax.rem(z + k, NZ), ep)

    for h in range(PARTS):
        @pl.when(inner)
        def _(h=h):
            line_own(0, far1, h).start()

        line_own(1, near, h).start()
    for k in range(1, NZ):
        icopy(k).start()
    idxl[z] = idx[...]
    xl[z] = tok[...]

    upper = jnp.where(iota((T, T), 0) < iota((T, T), 1), 1.0, 0.0).astype(BF)

    def codes(ids, first, n):
        eid = iota((n, T), 0) + first
        hit = jnp.zeros((n, T), F32)
        for j in range(6):
            hit = hit + jnp.where(ids[j : j + 1, :] == eid, 1.0, 0.0)
        rank = jnp.dot(hit.astype(BF), upper, preferred_element_type=F32)
        return jnp.where(hit > 0.5, rank, -1.0).astype(BF)

    def s_copy(b, k, h):
        d = lax.rem(ep + k, NE)
        return remote(
            sel.at[b, d, :, span(h)], xr.at[b * NE + ep, :, span(h)], ssend.at[b, k - 1, h],
            srecv.at[b * NE + ep, h], z, d
        )

    def picks(b):
        code = codes(idxl[b], z * NE * LE, NE * LE)
        r = iota((PLANE, NE * LE), 0)
        ex = jnp.where(div_cap(r) == iota((PLANE, NE * LE), 1), 1.0, 0.0).astype(BF)
        code_r = jnp.dot(ex, code, preferred_element_type=F32)
        r = iota((PLANE, T), 0)
        slot = (r - div_cap(r) * CAP).astype(F32)
        pick[...] = jnp.where(code_r == slot, 1.0, 0.0).astype(BF)

    def select(b, h):
        wide = D // PARTS // 2

        def cols(c, _):
            cs = pl.ds(pl.multiple_of(h * (D // PARTS) + c * wide, 128), wide)
            rows = jnp.dot(pick[...], xl[b, :, cs], preferred_element_type=F32).astype(BF)
            sel[b, :, :, cs] = rows.reshape(NE, BLK, wide)
            return 0

        lax.fori_loop(0, 2, cols, 0)
        for k in range(1, NE):
            s_copy(b, k, h).start()
        xr[b * NE + ep, :, span(h)] = sel[b, ep, :, span(h)]

    def idx_wait(b):
        remote(idx, idxl.at[b], isend.at[0], irecv.at[b], z, ep).wait_recv()

    picks(z)
    for h in range(PARTS):
        select(z, h)

    n_exp = NDEV * LE
    idx_v, gates_v = idx[...], gates[...]
    code = codes(idx_v, 0, n_exp)
    eid = iota((n_exp, T), 0)
    gate = jnp.zeros((n_exp, T), F32)
    for j in range(6):
        gate = gate + jnp.where(idx_v[j : j + 1, :] == eid, gates_v[j : j + 1, :], 0.0)
    g_hi = gate.astype(BF)
    rest = gate - g_hi.astype(F32)
    g_mid = rest.astype(BF)
    g_lo = (rest - g_mid.astype(F32)).astype(BF)

    def spread(a, ex):
        return lax.dot_general(a, ex, (((0,), (0,)), ((), ())), preferred_element_type=F32)

    for b in range(NZ):
        c = iota((n_exp, PLANE), 1)
        ex = jnp.where(div_cap(c) + b * NE * LE == iota((n_exp, PLANE), 0), 1.0, 0.0).astype(BF)
        c = iota((T, PLANE), 1)
        slot = (c - div_cap(c) * CAP).astype(F32)
        on = spread(code, ex) == slot
        for q, part in enumerate((g_hi, g_mid, g_lo)):
            gm[q, b] = jnp.where(on, spread(part, ex), 0.0).astype(BF)

    def pick_plane(a, b):
        return jnp.where(inner, a, b)

    q0, q1, q2 = pick_plane(far1, near), pick_plane(far2, far1), pick_plane(near, far2)
    for h in range(PARTS):
        line_wait(q0, h)

        @pl.when(inner)
        def _(h=h):
            line(far1, 2, near, h).start()
            line_wait(near, h)
            line(near, 3, far1, h).start()

        if h == 0:
            idx_wait(q0)
            picks(q0)
        select(q0, h)

    for h in range(PARTS):
        if h == 0:
            idx_wait(q1)
            picks(q1)
        line_wait(q1, h)

        @pl.when(inner)
        def _(h=h):
            line(far2, 4, near, h).start()

        select(q1, h)

    def last_block():
        idx_wait(q2)
        picks(q2)
        for h in range(PARTS):
            @pl.when(edge)
            def _(h=h):
                line_wait(q2, h)

            select(q2, h)

    pl.when(inner)(last_block)

    def rows_wait(b):
        for k in range(1, NE):
            i = b * NE + lax.rem(ep + k, NE)
            for h in range(PARTS):
                at = xr.at[i, :, span(h)]
                remote(at, at, ssend.at[0, 0, 0], srecv.at[i, h], z, ep).wait_recv()

    def across(k):
        return lax.rem(lax.div(ep, 2) + k // 2, 2) * 2 + lax.rem(lax.rem(ep, 2) + k % 2, 2)

    def y_copy(zz, ee, e, desc):
        m = zz * NE + ee
        rows = pl.ds(*piece(e, desc))
        return remote(ys.at[m, rows], yr.at[me, rows], ysend.at[e, m], yrecv.at[e, me], zz, ee)

    def experts(p0, p1, n_pass):
        desc = n_pass == 1
        rows_wait(p0)
        rows_wait(p1)

        def step(i, ring, total, copies, before):
            if before:
                if n_pass == 0:
                    for cp in copies(i):
                        cp.wait()
                else:
                    @pl.when(i < total - ring if desc else i >= ring)
                    def _():
                        for cp in copies(i):
                            cp.wait()
            else:
                nxt = i - ring if desc else i + ring

                @pl.when(nxt >= 0 if desc else nxt < total)
                def _():
                    for cp in copies(nxt):
                        cp.start()

        for e in reversed(range(LE)) if desc else range(LE):
            win = WINDOWS[e]
            for s, p in enumerate((p0, p1)):
                def gather(m, _, s=s, p=p):
                    rows = pl.ds(pl.multiple_of(s * NE * 16 + m * 16, 16), 16)
                    a_buf[rows, :] = xr[p * NE + m, win : win + 16, :]
                    return 0

                lax.fori_loop(0, NE, gather, 0)

            def gate_up(c, _):
                c = n_f - 1 - c if desc else c
                i = e * n_f + c
                slot = lax.rem(i, NG)
                step(i, NG, LE * n_f, gu_copies, True)
                a = a_buf[...]
                g = jnp.dot(a, gu[slot, 0], preferred_element_type=F32)
                u = jnp.dot(a, gu[slot, 1], preferred_element_type=F32)
                h_buf[:, pl.ds(pl.multiple_of(c * FC, FC), FC)] = (jax.nn.silu(g) * u).astype(BF)
                step(i, NG, LE * n_f, gu_copies, False)
                return 0

            lax.fori_loop(0, n_f, gate_up, 0)

            def down_proj(c, _):
                c = n_d - 1 - c if desc else c
                i = e * n_d + c
                slot = lax.rem(i, ND)
                step(i, ND, LE * n_d, d_copies, True)
                y = jnp.dot(h_buf[...], wdb[slot], preferred_element_type=F32).reshape(2, NE, 16, DC)
                cs = pl.ds(pl.multiple_of(c * DC, DC), DC)
                second = (e % 2 == 0) == desc
                for s, p in enumerate((p0, p1)):
                    to = pl.ds(p * NE, NE)
                    if not second:
                        ys[to, win : win + 16, cs] = y[s].astype(BF)
                    elif e % 2:
                        old = ys[to, win : win + 8, cs].astype(F32)
                        keep = iota((NE, 8, DC), 1) < 4
                        ys[to, win : win + 8, cs] = jnp.where(keep, old, y[s, :, :8]).astype(BF)
                        ys[to, win + 8 : win + 16, cs] = y[s, :, 8:].astype(BF)
                    else:
                        old = ys[to, win + 8 : win + 16, cs].astype(F32)
                        keep = iota((NE, 8, DC), 1) >= 4
                        ys[to, win + 8 : win + 16, cs] = jnp.where(keep, old, y[s, :, 8:]).astype(BF)
                        ys[to, win : win + 8, cs] = y[s, :, :8].astype(BF)
                step(i, ND, LE * n_d, d_copies, False)
                return 0

            lax.fori_loop(0, n_d, down_proj, 0)

            for k in range(NE):
                y_copy(p0, across(k), e, desc).start()
            for k in range(NE):
                if k:
                    y_copy(p1, across(k), e, desc).start()
                else:
                    @pl.when(p1 != z)
                    def _():
                        y_copy(p1, ep, e, desc).start()
            if n_pass == 0 and e == LE - 2:
                pl.when(edge)(last_block)

    experts(pick_plane(far1, near), pick_plane(far2, z), 0)
    experts(pick_plane(near, far2), pick_plane(z, far1), 1)

    yr[me] = ys[me]

    def y_wait(i, desc):
        for e in range(LE):
            rows = pl.ds(*piece(e, desc))
            remote(yr.at[i, rows], yr.at[i, rows], ysend.at[0, 0], yrecv.at[e, i], z, ep).wait_recv()

    late_in = (inner, edge, z < 0, z >= 0)
    late_out = (inner, inner, edge, edge)

    for n, b in enumerate((z, near, far1, far2)):
        for k in range(1 if n == 0 else 0, NE):
            i = b * NE + (lax.rem(ep + k, NE) if n == 0 else k)

            @pl.when(late_in[n])
            def _(i=i):
                y_wait(i, True)

            @pl.when(jnp.logical_not(late_in[n]))
            def _(i=i):
                y_wait(i, False)

        def mix(c, _):
            cs = pl.ds(pl.multiple_of(c * DC, DC), DC)
            rows = yr[pl.ds(b * NE, NE), :, cs].reshape(PLANE, DC)
            s = tok[:, cs].astype(F32) if n == 0 else acc[:, cs]
            for q in range(3):
                s = s + jnp.dot(gm[q, b], rows, preferred_element_type=F32)
            if n < NZ - 1:
                acc[:, cs] = s
            else:
                out[:, cs] = s.astype(BF)
            return 0

        lax.fori_loop(0, n_d, mix, 0)

    for k in range(1, NZ):
        icopy(k).wait_send()
    for b in range(NZ):
        for k in range(1, NE):
            for h in range(PARTS):
                s_copy(b, k, h).wait_send()
    for h in range(PARTS):
        line_own(1, near, h).wait_send()

        @pl.when(inner)
        def _(h=h):
            line_own(0, far1, h).wait_send()
            line(far1, 2, near, h).wait_send()
            line(near, 3, far1, h).wait_send()
            line(far2, 4, near, h).wait_send()

    for n, b in enumerate((z, near, far1, far2)):
        for k in range(1 if n == 0 else 0, NE):
            d = lax.rem(ep + k, NE) if n == 0 else k
            for desc in (False, True):
                @pl.when(late_out[n] if desc else jnp.logical_not(late_out[n]))
                def _(b=b, d=d, desc=desc):
                    for e in range(LE):
                        y_copy(b, d, e, desc).wait_send()


def solution(mesh):
    row_spec = P(('dp', 'ep2', 'ep'), None)
    weight_spec = P(('ep2', 'ep'), None, None)

    def local_step(tokens, expert_idx, gates, w_gate, w_up, w_down):
        T, D = tokens.shape
        F = w_gate.shape[2]
        vm = pl.BlockSpec(memory_space=pltpu.VMEM)
        hbm = pl.BlockSpec(memory_space=pl.ANY)
        dma = pltpu.SemaphoreType.DMA
        return pl.pallas_call(
            kernel,
            name="moe",
            out_shape=jax.ShapeDtypeStruct((T, D), BF),
            in_specs=[vm, vm, vm, hbm, hbm, hbm],
            out_specs=vm,
            scratch_shapes=[
                pltpu.VMEM((NZ, T, D), BF),
                pltpu.VMEM((NZ, 6, T), jnp.int32),
                pltpu.VMEM((NZ, NE, BLK, D), BF),
                pltpu.VMEM((NDEV, BLK, D), BF),
                pltpu.VMEM((2 * NE * 16, D), BF),
                pltpu.VMEM((2 * NE * 16, F), BF),
                pltpu.VMEM((NDEV, BLK, D), BF),
                pltpu.VMEM((NDEV, BLK, D), BF),
                pltpu.VMEM((3, NZ, T, PLANE), BF),
                pltpu.VMEM((T, D), F32),
                pltpu.VMEM((PLANE, T), BF),
                pltpu.VMEM((NG, 2, D, FC), BF),
                pltpu.VMEM((ND, F, DC), BF),
                dma((NG, 2)),
                dma((ND,)),
                dma((NZ - 1,)),
                dma((NZ,)),
                dma((5, PARTS)),
                dma((NZ, PARTS)),
                dma((NZ, NE - 1, PARTS)),
                dma((NDEV, PARTS)),
                dma((LE, NDEV)),
                dma((LE, NDEV)),
            ],
            compiler_params=pltpu.CompilerParams(
                collective_id=0, has_side_effects=True, vmem_limit_bytes=67043328
            ),
        )(tokens, expert_idx.T, gates.T, w_gate, w_up, w_down)

    return jax.shard_map(local_step, mesh=mesh, in_specs=(row_spec, row_spec, row_spec, weight_spec, weight_spec, weight_spec), out_specs=row_spec, check_vma=False)
```

```python
import functools

import jax
import jax.numpy as jnp
from jax import lax
from jax.experimental import pallas as pl
from jax.experimental.pallas import tpu as pltpu
from jax.sharding import PartitionSpec as P

MESH = pl.DeviceIdType.MESH
BF = jnp.bfloat16
F32 = jnp.float32
NZ = 4
NE = 4
NDEV = NZ * NE
LE = 4
CAP = 12
BLK = LE * CAP
PLANE = NE * BLK
HALF = BLK // 2
WINDOWS = (0, 8, 24, 32)
FC = 512
DC = 512
NG = 5
ND = 6
PARTS = 2


def iota(shape, dim):
    return lax.broadcasted_iota(jnp.int32, shape, dim)


def div_cap(v):
    return (v * 43691) >> 19


def piece(e, desc):
    base = (e // 2) * HALF
    if desc:
        return (base + 16, 8) if e % 2 else (base, 16)
    return (base + 8, 16) if e % 2 else (base, 8)


def kernel(tok, idx, gates, wg, wu, wd, out, xl, idxl, sel, xr, a_buf, h_buf, ys, yr, gm, acc, pick, gu, wdb,
           gsem, dsem, isend, irecv, lsend, lrecv, ssend, srecv, ysend, yrecv):
    T, D = tok.shape
    F = wg.shape[2]
    n_f, n_d = F // FC, D // DC
    dp, z, ep = lax.axis_index("dp"), lax.axis_index("ep2"), lax.axis_index("ep")
    me = z * NE + ep
    low = z < NZ // 2
    inner = (z == 1) | (z == 2)
    edge = jnp.logical_not(inner)
    near = jnp.where(low, 1 - z, 5 - z)
    far1 = jnp.where(low, 2, 1)
    far2 = jnp.where(low, 3, 0)

    def remote(src, dst, ss, rs, zz, ee):
        return pltpu.make_async_remote_copy(
            src_ref=src, dst_ref=dst, send_sem=ss, recv_sem=rs, device_id=(dp, zz, ee), device_id_type=MESH
        )

    def gu_copies(i):
        e, c, slot = lax.div(i, n_f), lax.rem(i, n_f), lax.rem(i, NG)
        cols = pl.ds(pl.multiple_of(c * FC, FC), FC)
        return (
            pltpu.make_async_copy(wg.at[e, :, cols], gu.at[slot, 0], gsem.at[slot, 0]),
            pltpu.make_async_copy(wu.at[e, :, cols], gu.at[slot, 1], gsem.at[slot, 1]),
        )

    def d_copies(i):
        e, c, slot = lax.div(i, n_d), lax.rem(i, n_d), lax.rem(i, ND)
        cols = pl.ds(pl.multiple_of(c * DC, DC), DC)
        return (pltpu.make_async_copy(wd.at[e, :, cols], wdb.at[slot], dsem.at[slot]),)

    barrier = pltpu.get_barrier_semaphore()
    for k in range(1, NDEV):
        peer = lax.rem(me + k, NDEV)
        pl.semaphore_signal(barrier, inc=1, device_id=(dp, lax.div(peer, NE), lax.rem(peer, NE)), device_id_type=MESH)
    for i in range(NG):
        for cp in gu_copies(jnp.int32(i)):
            cp.start()
    for i in range(ND):
        for cp in d_copies(jnp.int32(i)):
            cp.start()

    pl.semaphore_wait(barrier, NDEV - 1)

    def span(h):
        return pl.ds(h * (D // PARTS), D // PARTS)

    def line(b, n, to, h):
        at = xl.at[b, :, span(h)]
        return remote(at, at, lsend.at[n, h], lrecv.at[b, h], to, ep)

    def line_own(n, to, h):
        return remote(tok.at[:, span(h)], xl.at[z, :, span(h)], lsend.at[n, h], lrecv.at[z, h], to, ep)

    def line_wait(b, h):
        line(b, 0, z, h).wait_recv()

    def icopy(k):
        return remote(idx, idxl.at[z], isend.at[k - 1], irecv.at[z], lax.rem(z + k, NZ), ep)

    for h in range(PARTS):
        @pl.when(inner)
        def _(h=h):
            line_own(0, far1, h).start()

        line_own(1, near, h).start()
    for k in range(1, NZ):
        icopy(k).start()
    idxl[z] = idx[...]
    xl[z] = tok[...]

    upper = jnp.where(iota((T, T), 0) < iota((T, T), 1), 1.0, 0.0).astype(BF)

    def codes(ids, first, n):
        eid = iota((n, T), 0) + first
        hit = jnp.zeros((n, T), F32)
        for j in range(6):
            hit = hit + jnp.where(ids[j : j + 1, :] == eid, 1.0, 0.0)
        rank = jnp.dot(hit.astype(BF), upper, preferred_element_type=F32)
        return jnp.where(hit > 0.5, rank, -1.0).astype(BF)

    def s_copy(b, k, h):
        d = lax.rem(ep + k, NE)
        return remote(
            sel.at[b, d, :, span(h)], xr.at[b * NE + ep, :, span(h)], ssend.at[b, k - 1, h],
            srecv.at[b * NE + ep, h], z, d
        )

    def picks(b):
        code = codes(idxl[b], z * NE * LE, NE * LE)
        r = iota((PLANE, NE * LE), 0)
        ex = jnp.where(div_cap(r) == iota((PLANE, NE * LE), 1), 1.0, 0.0).astype(BF)
        code_r = jnp.dot(ex, code, preferred_element_type=F32)
        r = iota((PLANE, T), 0)
        slot = (r - div_cap(r) * CAP).astype(F32)
        pick[...] = jnp.where(code_r == slot, 1.0, 0.0).astype(BF)

    def select(b, h):
        wide = D // PARTS // 2

        def cols(c, _):
            cs = pl.ds(pl.multiple_of(h * (D // PARTS) + c * wide, 128), wide)
            rows = jnp.dot(pick[...], xl[b, :, cs], preferred_element_type=F32).astype(BF)
            sel[b, :, :, cs] = rows.reshape(NE, BLK, wide)
            return 0

        lax.fori_loop(0, 2, cols, 0)
        for k in range(1, NE):
            s_copy(b, k, h).start()
        xr[b * NE + ep, :, span(h)] = sel[b, ep, :, span(h)]

    def idx_wait(b):
        remote(idx, idxl.at[b], isend.at[0], irecv.at[b], z, ep).wait_recv()

    picks(z)
    for h in range(PARTS):
        select(z, h)

    n_exp = NDEV * LE
    idx_v, gates_v = idx[...], gates[...]
    code = codes(idx_v, 0, n_exp)
    eid = iota((n_exp, T), 0)
    gate = jnp.zeros((n_exp, T), F32)
    for j in range(6):
        gate = gate + jnp.where(idx_v[j : j + 1, :] == eid, gates_v[j : j + 1, :], 0.0)
    g_hi = gate.astype(BF)
    rest = gate - g_hi.astype(F32)
    g_mid = rest.astype(BF)
    g_lo = (rest - g_mid.astype(F32)).astype(BF)

    def spread(a, ex):
        return lax.dot_general(a, ex, (((0,), (0,)), ((), ())), preferred_element_type=F32)

    for b in range(NZ):
        c = iota((n_exp, PLANE), 1)
        ex = jnp.where(div_cap(c) + b * NE * LE == iota((n_exp, PLANE), 0), 1.0, 0.0).astype(BF)
        c = iota((T, PLANE), 1)
        slot = (c - div_cap(c) * CAP).astype(F32)
        on = spread(code, ex) == slot
        for q, part in enumerate((g_hi, g_mid, g_lo)):
            gm[q, b] = jnp.where(on, spread(part, ex), 0.0).astype(BF)

    def pick_plane(a, b):
        return jnp.where(inner, a, b)

    q0, q1, q2 = pick_plane(far1, near), pick_plane(far2, far1), pick_plane(near, far2)
    for h in range(PARTS):
        line_wait(q0, h)

        @pl.when(inner)
        def _(h=h):
            line(far1, 2, near, h).start()
            line_wait(near, h)
            line(near, 3, far1, h).start()

        if h == 0:
            idx_wait(q0)
            picks(q0)
        select(q0, h)

    for h in range(PARTS):
        if h == 0:
            idx_wait(q1)
            picks(q1)
        line_wait(q1, h)

        @pl.when(inner)
        def _(h=h):
            line(far2, 4, near, h).start()

        select(q1, h)

    def last_block():
        idx_wait(q2)
        picks(q2)
        for h in range(PARTS):
            @pl.when(edge)
            def _(h=h):
                line_wait(q2, h)

            select(q2, h)

    pl.when(inner)(last_block)

    def rows_wait(b):
        for k in range(1, NE):
            i = b * NE + lax.rem(ep + k, NE)
            for h in range(PARTS):
                at = xr.at[i, :, span(h)]
                remote(at, at, ssend.at[0, 0, 0], srecv.at[i, h], z, ep).wait_recv()

    def across(k):
        return lax.rem(lax.div(ep, 2) + lax.rem(ep, 2) + k // 2, 2) * 2 + lax.rem(lax.rem(ep, 2) + k % 2, 2)

    def y_copy(zz, ee, e, desc):
        m = zz * NE + ee
        rows = pl.ds(*piece(e, desc))
        return remote(ys.at[m, rows], yr.at[me, rows], ysend.at[e, m], yrecv.at[e, me], zz, ee)

    def experts(p0, p1, n_pass):
        desc = n_pass == 1
        rows_wait(p0)
        rows_wait(p1)

        def step(i, ring, total, copies, before):
            if before:
                if n_pass == 0:
                    for cp in copies(i):
                        cp.wait()
                else:
                    @pl.when(i < total - ring if desc else i >= ring)
                    def _():
                        for cp in copies(i):
                            cp.wait()
            else:
                nxt = i - ring if desc else i + ring

                @pl.when(nxt >= 0 if desc else nxt < total)
                def _():
                    for cp in copies(nxt):
                        cp.start()

        for e in reversed(range(LE)) if desc else range(LE):
            win = WINDOWS[e]
            for s, p in enumerate((p0, p1)):
                def gather(m, _, s=s, p=p):
                    rows = pl.ds(pl.multiple_of(s * NE * 16 + m * 16, 16), 16)
                    a_buf[rows, :] = xr[p * NE + m, win : win + 16, :]
                    return 0

                lax.fori_loop(0, NE, gather, 0)

            def gate_up(c, _):
                c = n_f - 1 - c if desc else c
                i = e * n_f + c
                slot = lax.rem(i, NG)
                step(i, NG, LE * n_f, gu_copies, True)
                a = a_buf[...]
                g = jnp.dot(a, gu[slot, 0], preferred_element_type=F32)
                u = jnp.dot(a, gu[slot, 1], preferred_element_type=F32)
                h_buf[:, pl.ds(pl.multiple_of(c * FC, FC), FC)] = (jax.nn.silu(g) * u).astype(BF)
                step(i, NG, LE * n_f, gu_copies, False)
                return 0

            lax.fori_loop(0, n_f, gate_up, 0)

            def down_proj(c, _):
                c = n_d - 1 - c if desc else c
                i = e * n_d + c
                slot = lax.rem(i, ND)
                step(i, ND, LE * n_d, d_copies, True)
                y = jnp.dot(h_buf[...], wdb[slot], preferred_element_type=F32).reshape(2, NE, 16, DC)
                cs = pl.ds(pl.multiple_of(c * DC, DC), DC)
                second = (e % 2 == 0) == desc
                for s, p in enumerate((p0, p1)):
                    to = pl.ds(p * NE, NE)
                    if not second:
                        ys[to, win : win + 16, cs] = y[s].astype(BF)
                    elif e % 2:
                        old = ys[to, win : win + 8, cs].astype(F32)
                        keep = iota((NE, 8, DC), 1) < 4
                        ys[to, win : win + 8, cs] = jnp.where(keep, old, y[s, :, :8]).astype(BF)
                        ys[to, win + 8 : win + 16, cs] = y[s, :, 8:].astype(BF)
                    else:
                        old = ys[to, win + 8 : win + 16, cs].astype(F32)
                        keep = iota((NE, 8, DC), 1) >= 4
                        ys[to, win + 8 : win + 16, cs] = jnp.where(keep, old, y[s, :, 8:]).astype(BF)
                        ys[to, win : win + 8, cs] = y[s, :, :8].astype(BF)
                step(i, ND, LE * n_d, d_copies, False)
                return 0

            lax.fori_loop(0, n_d, down_proj, 0)

            for k in range(NE):
                y_copy(p0, across(k), e, desc).start()
            for k in range(NE):
                @pl.when((p1 != z) | (across(k) != ep))
                def _(k=k):
                    y_copy(p1, across(k), e, desc).start()
            if n_pass == 0 and e == LE - 2:
                pl.when(edge)(last_block)

    experts(pick_plane(far1, near), pick_plane(far2, z), 0)
    experts(pick_plane(near, far2), pick_plane(z, far1), 1)

    yr[me] = ys[me]

    def y_wait(i, desc):
        for e in range(LE):
            rows = pl.ds(*piece(e, desc))
            remote(yr.at[i, rows], yr.at[i, rows], ysend.at[0, 0], yrecv.at[e, i], z, ep).wait_recv()

    late_in = (inner, edge, z < 0, z >= 0)
    late_out = (inner, inner, edge, edge)

    for n, b in enumerate((z, near, far1, far2)):
        for k in range(1 if n == 0 else 0, NE):
            i = b * NE + (lax.rem(ep + k, NE) if n == 0 else k)

            @pl.when(late_in[n])
            def _(i=i):
                y_wait(i, True)

            @pl.when(jnp.logical_not(late_in[n]))
            def _(i=i):
                y_wait(i, False)

        def mix(c, _):
            cs = pl.ds(pl.multiple_of(c * DC, DC), DC)
            rows = yr[pl.ds(b * NE, NE), :, cs].reshape(PLANE, DC)
            s = tok[:, cs].astype(F32) if n == 0 else acc[:, cs]
            for q in range(3):
                s = s + jnp.dot(gm[q, b], rows, preferred_element_type=F32)
            if n < NZ - 1:
                acc[:, cs] = s
            else:
                out[:, cs] = s.astype(BF)
            return 0

        lax.fori_loop(0, n_d, mix, 0)

    for k in range(1, NZ):
        icopy(k).wait_send()
    for b in range(NZ):
        for k in range(1, NE):
            for h in range(PARTS):
                s_copy(b, k, h).wait_send()
    for h in range(PARTS):
        line_own(1, near, h).wait_send()

        @pl.when(inner)
        def _(h=h):
            line_own(0, far1, h).wait_send()
            line(far1, 2, near, h).wait_send()
            line(near, 3, far1, h).wait_send()
            line(far2, 4, near, h).wait_send()

    for n, b in enumerate((z, near, far1, far2)):
        for k in range(1 if n == 0 else 0, NE):
            d = lax.rem(ep + k, NE) if n == 0 else k
            for desc in (False, True):
                @pl.when(late_out[n] if desc else jnp.logical_not(late_out[n]))
                def _(b=b, d=d, desc=desc):
                    for e in range(LE):
                        y_copy(b, d, e, desc).wait_send()


def solution(mesh):
    row_spec = P(('dp', 'ep2', 'ep'), None)
    weight_spec = P(('ep2', 'ep'), None, None)

    def local_step(tokens, expert_idx, gates, w_gate, w_up, w_down):
        T, D = tokens.shape
        F = w_gate.shape[2]
        vm = pl.BlockSpec(memory_space=pltpu.VMEM)
        hbm = pl.BlockSpec(memory_space=pl.ANY)
        dma = pltpu.SemaphoreType.DMA
        return pl.pallas_call(
            kernel,
            name="moe",
            out_shape=jax.ShapeDtypeStruct((T, D), BF),
            in_specs=[vm, vm, vm, hbm, hbm, hbm],
            out_specs=vm,
            scratch_shapes=[
                pltpu.VMEM((NZ, T, D), BF),
                pltpu.VMEM((NZ, 6, T), jnp.int32),
                pltpu.VMEM((NZ, NE, BLK, D), BF),
                pltpu.VMEM((NDEV, BLK, D), BF),
                pltpu.VMEM((2 * NE * 16, D), BF),
                pltpu.VMEM((2 * NE * 16, F), BF),
                pltpu.VMEM((NDEV, BLK, D), BF),
                pltpu.VMEM((NDEV, BLK, D), BF),
                pltpu.VMEM((3, NZ, T, PLANE), BF),
                pltpu.VMEM((T, D), F32),
                pltpu.VMEM((PLANE, T), BF),
                pltpu.VMEM((NG, 2, D, FC), BF),
                pltpu.VMEM((ND, F, DC), BF),
                dma((NG, 2)),
                dma((ND,)),
                dma((NZ - 1,)),
                dma((NZ,)),
                dma((5, PARTS)),
                dma((NZ, PARTS)),
                dma((NZ, NE - 1, PARTS)),
                dma((NDEV, PARTS)),
                dma((LE, NDEV)),
                dma((LE, NDEV)),
            ],
            compiler_params=pltpu.CompilerParams(
                collective_id=0, has_side_effects=True, vmem_limit_bytes=67043328
            ),
        )(tokens, expert_idx.T, gates.T, w_gate, w_up, w_down)

    return jax.shard_map(local_step, mesh=mesh, in_specs=(row_spec, row_spec, row_spec, weight_spec, weight_spec, weight_spec), out_specs=row_spec, check_vma=False)
```
